256 devices in a mesh: samp: 4 (over x), gx: 8 (over y, core), gy: 8 (over z).
Axes of the slice: x: 4, y: 4, z: 8, core: 2. Of those that a mesh axis runs over, the one named last changes fastest.
Arguments:
- load: float32 [4, 2, 1024, 4096], P('samp', None, 'gx', 'gy'), parts along dimension 0, may hold values from -6 to 6
- material: int32 [4, 128, 512], P('samp', 'gx', 'gy'), parts along dimension 0, may hold values from 0 to 7
- lame_table: float32 [2, 8], replicated, may hold values from 0.3 to 6
Outputs:
- solution: float32 [4, 2, 1024, 4096], P('samp', None, 'gx', 'gy'), parts along dimension 0
- residual: float32 [4, 2, 1024, 4096], P('samp', None, 'gx', 'gy'), parts along dimension 0
The draws below stay inside these ranges and needn't reach their ends.
There are 4 independent parts, one for each index of `samp`. The reference program is written for one: setup_inputs(seed, part) draws one part's arguments, and reference() takes and returns one part's arrays. A program takes and returns all parts, laid end to end along the dimension named above; an argument that names none is the same for every part. Nothing has to cross between parts.
All inputs are finite; a program needn't handle non-finite values.
Results may differ from the reference program's by a relative error of at most 0.0003.
Values sent between devices are 32-bit elements; how exact they have to be, the bound alone decides.
A program may use at most 64 MiB of HBM per device.

```python
import math
import jax
import jax.numpy as jnp

SAMPLES = 1
TILE = 8
CLASSES = 8
ITERS = 4
NX = 1024
NY = 4096


def plant(result, stream_key, low, top_value):
    spot = [jax.random.randint(jax.random.fold_in(stream_key, axis), (), 0, length) for axis, length in enumerate(result.shape)]
    longest = result.shape.index(max(result.shape))
    beside = spot[:longest] + [(spot[longest] + 1) % result.shape[longest]] + spot[longest + 1:]
    return result.at[tuple(spot)].set(low).at[tuple(beside)].set(top_value)


def steps_of(own_key, shape, split, smallest, top_value):
    gain = 1.0
    for position, blocks in split:
        heights = jax.random.uniform(jax.random.fold_in(jax.random.fold_in(own_key, 6), position), (blocks,), jnp.float32, smallest / len(split), top_value / len(split))
        gain = gain * jnp.repeat(jnp.exp(heights), shape[position] // blocks).reshape((-1,) + (1,) * (len(shape) - 1 - position))
    return gain


def centred(stream_key, shape, deviation, most, cuts=(), kind=jnp.bfloat16):
    entries = deviation * jax.random.normal(stream_key, shape, jnp.float32)
    if cuts:
        entries = entries * steps_of(stream_key, shape, cuts, -0.22, 0.18)
    return jnp.clip(entries, -most, most).astype(kind)


def setup_inputs(seed: int = 0, part: int = 0) -> dict:
    key_of = jax.random.split(jax.random.key(seed), 4)
    part_splits = jax.random.split(jax.random.fold_in(key_of[3], part), 4)
    return {
        "load": centred(part_splits[0], (SAMPLES, 2, NX, NY), 1.0, 6.0, ((2, 8), (3, 8)), jnp.float32),
        "material": plant(jax.random.randint(part_splits[1], (SAMPLES, NX // TILE, NY // TILE), 0, CLASSES), jax.random.fold_in(part_splits[1], 1), 0, CLASSES - 1).astype(jnp.int32),
        "lame_table": jnp.clip(jnp.exp(jax.random.uniform(key_of[2], (2, CLASSES), jnp.float32, math.log(0.3), math.log(6.0))), 0.3, 6.0),
    }


def cell_moduli(material, lame_table):
    classes = jnp.arange(CLASSES, dtype=jnp.int32)
    match = (material[..., None] == classes).astype(jnp.float32)
    lam = jnp.sum(match * lame_table[0], axis=-1)
    mu = jnp.sum(match * lame_table[1], axis=-1)

    def expand(tiles):
        count, rows, cols = tiles.shape
        wide = jnp.broadcast_to(tiles[:, :, None, :, None], (count, rows, TILE, cols, TILE))
        return wide.reshape(count, rows * TILE, cols * TILE)

    return expand(lam), expand(mu)


def cell_terms(nodes, lam, mu):
    low_low = nodes[..., :-1, :-1]
    high_low = nodes[..., 1:, :-1]
    low_high = nodes[..., :-1, 1:]
    high_high = nodes[..., 1:, 1:]
    along_x = 0.5 * ((high_low + high_high) - (low_low + low_high))
    along_y = 0.5 * ((low_high + high_high) - (low_low + high_low))
    strain_xx = along_x[:, 0]
    strain_yy = along_y[:, 1]
    shear = along_y[:, 0] + along_x[:, 1]
    stiff = lam + 2.0 * mu
    stress_xx = stiff * strain_xx + lam * strain_yy
    stress_yy = lam * strain_xx + stiff * strain_yy
    stress_xy = mu * shear
    plus = 0.5 * jnp.stack([stress_xx + stress_xy, stress_xy + stress_yy], axis=1)
    minus = 0.5 * jnp.stack([stress_xx - stress_xy, stress_xy - stress_yy], axis=1)
    return plus, minus


def operate(field, lam_pad, mu_pad):
    padded = jnp.pad(field, ((0, 0), (0, 0), (1, 1), (1, 1)))
    plus, minus = cell_terms(padded, lam_pad, mu_pad)
    forces = plus[..., :-1, :-1] - plus[..., 1:, 1:] + minus[..., :-1, 1:] - minus[..., 1:, :-1]
    return 0.05 * field + forces


def reference(load, material, lame_table):
    lam, mu = cell_moduli(material, lame_table)
    lam_pad = jnp.pad(lam, ((0, 0), (1, 0), (1, 0)))
    mu_pad = jnp.pad(mu, ((0, 0), (1, 0), (1, 0)))
    solution = jnp.zeros_like(load)
    residual = load
    w_vec = operate(residual, lam_pad, mu_pad)
    z_vec = jnp.zeros_like(load)
    q_vec = jnp.zeros_like(load)
    p_vec = jnp.zeros_like(load)
    gamma_prev = jnp.ones((load.shape[0],), jnp.float32)
    alpha_prev = jnp.ones((load.shape[0],), jnp.float32)
    for step in range(ITERS):
        gamma = jnp.sum(residual * residual, axis=(1, 2, 3))
        delta = jnp.sum(w_vec * residual, axis=(1, 2, 3))
        if step == 0:
            beta = jnp.zeros_like(gamma)
            alpha = gamma / delta
        else:
            beta = gamma / gamma_prev
            alpha = gamma / (delta - beta * gamma / alpha_prev)
        beta_b = beta[:, None, None, None]
        alpha_b = alpha[:, None, None, None]
        if step + 1 < ITERS:
            n_vec = operate(w_vec, lam_pad, mu_pad)
            z_vec = n_vec + beta_b * z_vec
        q_vec = w_vec + beta_b * q_vec
        p_vec = residual + beta_b * p_vec
        solution = solution + alpha_b * p_vec
        residual = residual - alpha_b * q_vec
        if step + 1 < ITERS:
            w_vec = w_vec - alpha_b * z_vec
        gamma_prev = gamma
        alpha_prev = alpha
    return solution, residual
```

```python
import functools

import jax
import jax.numpy as jnp
from jax import lax
from jax.experimental import pallas as pl
from jax.experimental.pallas import tpu as pltpu
from jax.sharding import PartitionSpec as P

TILE = 8
CLASSES = 8
ITERS = 4
LEVELS = ITERS
MASS = 0.05
SPREAD = 1.5
CENTRE = 1.5
DIAG = -CENTRE / SPREAD
MESH = pl.DeviceIdType.MESH
WAYS = [(dx, dy) for dx in (-1, 0, 1) for dy in (-1, 0, 1) if (dx, dy) != (0, 0)]
SIDE = 5
DIAGONAL = [w for w in WAYS if w[0] and w[1]]


def loop(count, body, carry, unroll=None):
    return lax.fori_loop(0, count, body, carry, unroll=count if unroll is None else unroll)


def kernel(
    nx, ny, load, material, table, out_x, out_r,
    v, vl, stress, moduli, compact, row_halo, col_send, col_halo, corner, mat_halo, slots_x, slots_y, own_sum,
    moments, send_sem, recv_sem, sum_send, sum_recv_x, sum_recv_y,
):
    rows, cols = load.shape[2], load.shape[3]
    tiles, planes = rows // 8, cols // 128
    mat_rows, mat_cols = material.shape[1], material.shape[2]
    extra = planes
    gx, gy = lax.axis_index("gx"), lax.axis_index("gy")
    has = {
        (-1, 0): gx > 0, (1, 0): gx < nx - 1, (0, -1): gy > 0, (0, 1): gy < ny - 1,
    }
    for dx, dy in DIAGONAL:
        has[dx, dy] = jnp.logical_and(has[dx, 0], has[0, dy])

    def at(dx, dy):
        return {"gx": lax.rem(gx + dx + nx, nx), "gy": lax.rem(gy + dy + ny, ny)}

    barrier = pltpu.get_barrier_semaphore()
    greeted = [(d, 0) for d in range(1, nx)] + [(0, d) for d in range(1, ny)] + DIAGONAL
    for way in greeted:
        pl.semaphore_signal(barrier, inc=1, device_id=at(*way), device_id_type=MESH)

    sub = lax.broadcasted_iota(jnp.int32, (8, 128), 0)
    lane = lax.broadcasted_iota(jnp.int32, (8, 128), 1)

    for c in range(2):
        col_send[0, c] = load[0, c, :, 0:128].T[0:8]
        col_send[1, c] = load[0, c, :, cols - 128 : cols].T[120:128]

    pl.semaphore_wait(barrier, len(greeted))

    def copies(index):
        dx, dy = WAYS[index]
        width = slice(0, cols) if dy == 0 else (slice(0, 128) if dy < 0 else slice(cols - 128, cols))
        strip = slice(0, 8) if dx < 0 else slice(rows - 8, rows)
        third = 1 - dy
        if dx == 0:
            mat_src, mat_rows_at = slice(0, mat_rows), slice(0, mat_rows)
            src = col_send.at[0 if dy < 0 else 1]
            dst = col_halo.at[:, slice(0, 8) if dy < 0 else slice(120, 128), :]
        else:
            mat_src = slice(0, 8) if dx < 0 else slice(mat_rows - 8, mat_rows)
            mat_rows_at = slice(mat_rows, mat_rows + 8) if dx < 0 else slice(mat_rows + 8, mat_rows + 16)
            src = load.at[0, :, strip, width]
            if dy == 0:
                dst = row_halo.at[0 if dx < 0 else 1]
            else:
                dst = corner.at[0 if dx < 0 else 1, 0 if dy > 0 else 1]
        field = pltpu.make_async_remote_copy(
            src_ref=src, dst_ref=dst, send_sem=send_sem.at[2 * index], recv_sem=recv_sem.at[2 * index],
            device_id=at(dx, dy), device_id_type=MESH,
        )
        classes = pltpu.make_async_remote_copy(
            src_ref=material.at[0, mat_src, :], dst_ref=mat_halo.at[third, mat_rows_at, :],
            send_sem=send_sem.at[2 * index + 1], recv_sem=recv_sem.at[2 * index + 1],
            device_id=at(dx, dy), device_id_type=MESH,
        )
        return field, classes

    order = sorted(range(len(WAYS)), key=lambda i: -abs(WAYS[i][0]) - abs(WAYS[i][1]) - abs(WAYS[i][1]))
    for index in order:
        @pl.when(has[WAYS[index]])
        def _(index=index):
            for copy in copies(index):
                copy.start()

    mean = 0.0
    for k in range(CLASSES):
        mean = mean + (table[0, k] + 3.0 * table[1, k])
    inv_s = jnp.full((8, 128), (SPREAD / CLASSES) * mean, jnp.float32)
    quarter = 0.25 / inv_s

    def looked_up(classes):
        lam = jnp.zeros(classes.shape, jnp.float32)
        mu = jnp.zeros(classes.shape, jnp.float32)
        for k in range(CLASSES):
            hit = classes == k
            lam = jnp.where(hit, table[0, k], lam)
            mu = jnp.where(hit, table[1, k], mu)
        return lam, mu

    spread_row = lax.broadcasted_iota(jnp.int32, (mat_cols, cols), 0)
    spread_col = lax.broadcasted_iota(jnp.int32, (mat_cols, cols), 1)
    spread = (spread_row == spread_col // TILE).astype(jnp.float32)

    def widened(classes):
        lam, mu = looked_up(classes)
        both = jnp.concatenate([lam, mu], axis=0)
        wide = jnp.dot(both, spread, precision=lax.Precision.HIGHEST, preferred_element_type=jnp.float32)
        return wide[: classes.shape[0]], wide[classes.shape[0] :]

    def put_moduli(place, lam, mu):
        k, r = place
        small = quarter * mu
        moduli[0, k, r, :] = quarter * lam
        moduli[1, k, r, :] = small + small
        moduli[2, k, r, :] = small

    lam, mu = widened(material[0])
    for t in range(tiles):
        for k in range(planes):
            part = slice(128 * k, 128 * (k + 1))
            put_moduli(
                (k, slice(8 * t, 8 * t + 8)),
                jnp.broadcast_to(lam[t : t + 1, part], (8, 128)),
                jnp.broadcast_to(mu[t : t + 1, part], (8, 128)),
            )

    def own(t, acc):
        r = pl.ds(pl.multiple_of(8 * t, 8), 8)
        for c in range(2):
            for k in range(planes):
                value = load[0, c, r, 128 * k : 128 * (k + 1)]
                v[0, c, k, r, :] = value
                acc = acc + value * value
        return acc

    moments[0] = loop(tiles, own, jnp.zeros((8, 128), jnp.float32))

    for index in range(len(WAYS)):
        dx, dy = WAYS[index]
        @pl.when(has[-dx, -dy])
        def _(index=index):
            for copy in copies(index):
                copy.wait_recv()

    low = sub < 4
    left_lanes = lane < 64
    inner_right = jnp.logical_and(lane < 4, has[0, 1])
    inner_left = jnp.logical_and(lane >= 124, has[0, -1])
    inner_lanes = jnp.logical_or(inner_right, inner_left)
    inner_below = jnp.logical_and(low, has[1, 0])
    inner_above = jnp.logical_and(sub >= 4, has[-1, 0])
    inner_subs = jnp.logical_or(inner_below, inner_above)
    inner_both = jnp.logical_and(inner_subs, inner_lanes)
    sub_mask = inner_subs.astype(jnp.float32)
    lane_mask = inner_lanes.astype(jnp.float32)
    both_mask = inner_both.astype(jnp.float32)
    halo = slice(rows, rows + 8)
    again = slice(rows + 8, rows + 16)
    for c in range(2):
        for k in range(planes):
            part = slice(128 * k, 128 * (k + 1))
            ring = jnp.where(low, row_halo[0, c, :, part], row_halo[1, c, :, part])
            v[0, c, k, halo, :] = jnp.where(inner_subs, ring, 0.0)
            v[0, c, k, again, :] = load[0, c, 0:8, part]
        beside = col_halo[c].T
        for t in range(tiles):
            value = jnp.where(inner_lanes, beside[8 * t : 8 * t + 8], 0.0)
            v[0, c, extra, 8 * t : 8 * t + 8, :] = value
            if t == 0:
                v[0, c, extra, again, :] = value
        below = jnp.where(left_lanes, corner[0, 1, c], corner[0, 0, c])
        above = jnp.where(left_lanes, corner[1, 1, c], corner[1, 0, c])
        v[0, c, extra, halo, :] = jnp.where(inner_both, jnp.where(low, below, above), 0.0)

    beyond = widened(mat_halo[1, mat_rows : mat_rows + 16, :])
    for k in range(planes):
        part = slice(128 * k, 128 * (k + 1))
        lam, mu = (
            jnp.where(
                inner_subs,
                jnp.where(low, jnp.broadcast_to(m[0:1, part], (8, 128)), jnp.broadcast_to(m[15:16, part], (8, 128))),
                0.0,
            )
            for m in beyond
        )
        put_moduli((k, halo), lam, mu)
    left, right = looked_up(mat_halo[0]), looked_up(mat_halo[2])
    for q in range(2):
        near = jnp.broadcast_to(right[q][:, 0:1], (mat_rows + 16, 128))
        far = jnp.broadcast_to(left[q][:, mat_cols - 1 : mat_cols], (mat_rows + 16, 128))
        wide_lane = lax.broadcasted_iota(jnp.int32, (mat_rows + 16, 128), 1)
        compact[q] = jnp.where(wide_lane < 64, near, far)
    for t in range(tiles):
        lam, mu = (
            jnp.where(inner_lanes, jnp.broadcast_to(compact[q, t : t + 1, :], (8, 128)), 0.0) for q in range(2)
        )
        put_moduli((extra, slice(8 * t, 8 * t + 8)), lam, mu)
    lam, mu = (
        jnp.where(
            inner_both,
            jnp.where(
                low,
                jnp.broadcast_to(compact[q, mat_rows : mat_rows + 1, :], (8, 128)),
                jnp.broadcast_to(compact[q, mat_rows + 15 : mat_rows + 16, :], (8, 128)),
            ),
            0.0,
        )
        for q in range(2)
    )
    put_moduli((extra, halo), lam, mu)

    last_lane, first_lane = lane == 127, lane == 0

    def shifted_left(parts):
        turned = [pltpu.roll(x, 127, 1) for x in parts]
        return [jnp.where(last_lane, turned[(k + 1) % SIDE], turned[k]) for k in range(SIDE)]

    def shifted_right(parts):
        turned = [pltpu.roll(x, 1, 1) for x in parts]
        return [jnp.where(first_lane, turned[k - 1], turned[k]) for k in range(SIDE)]

    def first_shift(t, carry):
        r = pl.ds(pl.multiple_of(8 * t, 8), 8)
        for c in range(2):
            for k, value in enumerate(shifted_left([v[0, c, k, r, :] for k in range(SIDE)])):
                vl[c, k, r, :] = value
        return carry

    loop(tiles + 2, first_shift, 0)

    def level_step(level, carry):
        diag = jnp.where(level == 0, 0.0, DIAG)

        def stresses(t, carry):
            base = pl.multiple_of(8 * t, 8)
            r, rr = pl.ds(base, 8), pl.ds(base + 1, 8)
            for k in range(SIDE):
                d = []
                for c in range(2):
                    u = vl[c, k, rr, :] - v[level, c, k, r, :]
                    w = v[level, c, k, rr, :] - vl[c, k, r, :]
                    d.append((u + w, u - w))
                (dx0, dy0), (dx1, dy1) = d
                common = moduli[0, k, r, :] * (dx0 + dy1)
                twice = moduli[1, k, r, :]
                s = pl.ds(base + 8, 8)
                stress[0, k, s, :] = common + twice * dx0
                stress[1, k, s, :] = moduli[2, k, r, :] * (dy0 + dx1)
                stress[2, k, s, :] = common + twice * dy1
            return carry

        loop(tiles + 1, stresses, 0)
        for q in range(3):
            for k in range(SIDE):
                stress[q, k, 0:8, :] = stress[q, k, rows + 8 : rows + 16, :]

        def forces(base, acc, border):
            r, s, b = pl.ds(base, 8), pl.ds(base + 8, 8), pl.ds(base + 7, 8)
            plain, moved = ([], []), ([], [])
            for k in range(SIDE):
                xx, xy, yy = stress[0, k, s, :], stress[1, k, s, :], stress[2, k, s, :]
                xx_b, xy_b, yy_b = stress[0, k, b, :], stress[1, k, b, :], stress[2, k, b, :]
                dxx, sxy, dxy, syy = xx_b - xx, xy_b + xy, xy_b - xy, yy_b + yy
                plain[0].append(dxx - sxy)
                moved[0].append(dxx + sxy)
                plain[1].append(dxy - syy)
                moved[1].append(dxy + syy)
            for c in range(2):
                new = []
                for k, value in enumerate(shifted_right(moved[c])):
                    old = v[level, c, k, r, :]
                    value = plain[c][k] + value + diag * old
                    if border:
                        value = value * (both_mask if k == extra else sub_mask)
                    elif k == extra:
                        value = value * lane_mask
                    else:
                        acc = (acc[0] + old * value, acc[1] + value * value)
                    v[level + 1, c, k, r, :] = value
                    new.append(value)
                for k, value in enumerate(shifted_left(new)):
                    vl[c, k, r, :] = value
            return acc

        zero = jnp.zeros((8, 128), jnp.float32)
        acc = loop(tiles, lambda t, acc: forces(pl.multiple_of(8 * t, 8), acc, False), (zero, zero))
        forces(rows, None, True)
        for c in range(2):
            for k in range(SIDE):
                v[level + 1, c, k, again, :] = v[level + 1, c, k, 0:8, :]
                vl[c, k, again, :] = vl[c, k, 0:8, :]
        moments[2 * level + 1] = acc[0]
        moments[2 * level + 2] = acc[1]
        return carry

    lax.fori_loop(0, LEVELS, level_step, 0)

    partial = jnp.sum(moments[0 : 2 * LEVELS], axis=1)
    partial = jnp.sum(partial, axis=1, keepdims=True)
    mine = jnp.sum(jnp.where(lane == sub, jnp.broadcast_to(partial, (8, 128)), 0.0), axis=0, keepdims=True)

    def summed(value, slots, here, size, way, first_sem, recv):
        slots[here] = value
        own_sum[first_sem] = value

        def copy(d):
            return pltpu.make_async_remote_copy(
                src_ref=own_sum.at[first_sem], dst_ref=slots.at[here],
                send_sem=sum_send.at[first_sem, d - 1], recv_sem=recv.at[d - 1],
                device_id=at(*way(d)), device_id_type=MESH,
            )

        for d in range(1, size):
            copy(d).start()
        for d in range(1, size):
            copy(d).wait_recv()
        total = slots[0]
        for d in range(1, size):
            total = total + slots[d]
        return total, copy

    mine, copy_x = summed(mine, slots_x, gx, nx, lambda d: (d, 0), 0, sum_recv_x)
    mine, copy_y = summed(mine, slots_y, gy, ny, lambda d: (0, d), 1, sum_recv_y)

    g = [jnp.broadcast_to(mine[:, k : k + 1], (8, 128)) for k in range(2 * LEVELS)]
    m = [g[0], g[1]]
    for k in range(2, 2 * LEVELS):
        m.append(g[k] + DIAG * m[k - 1])
    sigma0 = jnp.full((8, 128), MASS, jnp.float32)
    sigma = sigma0 + (CENTRE / SPREAD) * inv_s
    shift = [sigma0] + [sigma] * (2 * LEVELS - 2)
    rho, phi = dict(enumerate(m)), dict(enumerate(m))
    one, nil = jnp.ones((8, 128), jnp.float32), jnp.zeros((8, 128), jnp.float32)
    r_of, p_of, x_of = [one] + [nil] * LEVELS, [one] + [nil] * LEVELS, [nil] * LEVELS
    for t in range(ITERS):
        psi = {l: phi[l + 1] * inv_s + shift[l] * phi[l] for l in range(t, 2 * LEVELS - 1 - t)}
        alpha = rho[t] / psi[t]
        for k in range(t + 1):
            x_of[k] = x_of[k] + alpha * p_of[k]
        ap = [
            (p_of[k - 1] * inv_s if k else nil) + (shift[k] * p_of[k] if k <= t else nil) for k in range(t + 2)
        ]
        for k in range(t + 2):
            r_of[k] = r_of[k] - alpha * ap[k]
        if t + 1 < ITERS:
            new = {l: rho[l] - alpha * psi[l] for l in range(t + 1, 2 * LEVELS - 1 - t)}
            beta = -(alpha * inv_s) * new[t + 1] / rho[t]
            phi = {l: new[l] + beta * phi[l] for l in new}
            rho = new
            for k in range(t + 2):
                p_of[k] = r_of[k] + beta * p_of[k]

    def combine(t, carry):
        r = pl.ds(pl.multiple_of(8 * t, 8), 8)
        for c in range(2):
            for k in range(planes):
                basis = [v[l, c, k, r, :] for l in range(LEVELS + 1)]
                part = slice(128 * k, 128 * (k + 1))
                x = x_of[0] * basis[0]
                for l in range(1, LEVELS):
                    x = x + x_of[l] * basis[l]
                res = r_of[0] * basis[0]
                for l in range(1, LEVELS + 1):
                    res = res + r_of[l] * basis[l]
                out_x[0, c, r, part] = x
                out_r[0, c, r, part] = res
        return carry

    loop(tiles, combine, 0)

    for index in range(len(WAYS)):
        @pl.when(has[WAYS[index]])
        def _(index=index):
            for copy in copies(index):
                copy.wait_send()
    for d in range(1, nx):
        copy_x(d).wait_send()
    for d in range(1, ny):
        copy_y(d).wait_send()


def on_device(nx, ny, load, material, lame_table):
    rows, cols = load.shape[2], load.shape[3]
    mat_rows, mat_cols = material.shape[1], material.shape[2]
    planes = cols // 128
    vmem = pl.BlockSpec(memory_space=pltpu.VMEM)
    f32 = jnp.float32
    return pl.pallas_call(
        functools.partial(kernel, nx, ny),
        out_shape=[jax.ShapeDtypeStruct(load.shape, f32)] * 2,
        in_specs=[vmem, vmem, pl.BlockSpec(memory_space=pltpu.SMEM)],
        out_specs=[vmem, vmem],
        scratch_shapes=[
            pltpu.VMEM((LEVELS + 1, 2, planes + 1, rows + 16, 128), f32),
            pltpu.VMEM((2, planes + 1, rows + 16, 128), f32),
            pltpu.VMEM((3, planes + 1, rows + 16, 128), f32),
            pltpu.VMEM((3, planes + 1, rows + 8, 128), f32),
            pltpu.VMEM((2, mat_rows + 16, 128), f32),
            pltpu.VMEM((2, 2, 8, cols), f32),
            pltpu.VMEM((2, 2, 8, 128), f32),
            pltpu.VMEM((2, 128, rows), f32),
            pltpu.VMEM((2, 2, 2, 8, 128), f32),
            pltpu.VMEM((3, mat_rows + 16, mat_cols), jnp.int32),
            pltpu.VMEM((nx, 1, 128), f32),
            pltpu.VMEM((ny, 1, 128), f32),
            pltpu.VMEM((2, 1, 128), f32),
            pltpu.VMEM((2 * LEVELS + 1, 8, 128), f32),
            pltpu.SemaphoreType.DMA((2 * len(WAYS),)),
            pltpu.SemaphoreType.DMA((2 * len(WAYS),)),
            pltpu.SemaphoreType.DMA((2, max(nx, ny) - 1)),
            pltpu.SemaphoreType.DMA((nx - 1,)),
            pltpu.SemaphoreType.DMA((ny - 1,)),
        ],
        compiler_params=pltpu.CompilerParams(collective_id=0, has_side_effects=True),
    )(load, material, lame_table)


def solution(mesh):
    return jax.shard_map(
        functools.partial(on_device, mesh.shape["gx"], mesh.shape["gy"]),
        mesh=mesh,
        in_specs=(P("samp", None, "gx", "gy"), P("samp", "gx", "gy"), P()),
        out_specs=(P("samp", None, "gx", "gy"), P("samp", None, "gx", "gy")),
        check_vma=False,
    )
```

```python
import functools

import jax
import jax.numpy as jnp
from jax import lax
from jax.experimental import pallas as pl
from jax.experimental.pallas import tpu as pltpu
from jax.sharding import PartitionSpec as P

TILE = 8
CLASSES = 8
ITERS = 4
LEVELS = ITERS
MASS = 0.05
SPREAD = 1.5
CENTRE = 1.5
DIAG = -CENTRE / SPREAD
MESH = pl.DeviceIdType.MESH
WAYS = [(dx, dy) for dx in (-1, 0, 1) for dy in (-1, 0, 1) if (dx, dy) != (0, 0)]
SIDE = 5
DIAGONAL = [w for w in WAYS if w[0] and w[1]]


def loop(count, body, carry, unroll=None):
    return lax.fori_loop(0, count, body, carry, unroll=count if unroll is None else unroll)


def kernel(
    nx, ny, load_in, material_in, table_in, out_x, out_r,
    load, material, table, v, vl, stress, moduli, compact, row_halo, col_send, col_halo, corner, mat_halo, slots,
    own_sum, moments, load_sem, send_sem, recv_sem, sum_send, sum_recv, met,
):
    rows, cols = load.shape[2], load.shape[3]
    tiles, planes = rows // 8, cols // 128
    mat_rows, mat_cols = material.shape[1], material.shape[2]
    extra = planes
    gx, gy = lax.axis_index("gx"), lax.axis_index("gy")
    has = {
        (-1, 0): gx > 0, (1, 0): gx < nx - 1, (0, -1): gy > 0, (0, 1): gy < ny - 1,
    }
    for dx, dy in DIAGONAL:
        has[dx, dy] = jnp.logical_and(has[dx, 0], has[0, dy])

    def at(dx, dy):
        return {"gx": lax.rem(gx + dx + nx, nx), "gy": lax.rem(gy + dy + ny, ny)}

    barrier = pltpu.get_barrier_semaphore()
    for way in WAYS:
        pl.semaphore_signal(barrier, inc=1, device_id=at(*way), device_id_type=MESH)
    fetches = [
        pltpu.make_async_copy(load_in, load, load_sem.at[0]),
        pltpu.make_async_copy(material_in, material, load_sem.at[1]),
        pltpu.make_async_copy(table_in, table, load_sem.at[2]),
    ]
    for fetch in fetches:
        fetch.start()
    fetches[0].wait()

    sub = lax.broadcasted_iota(jnp.int32, (8, 128), 0)
    lane = lax.broadcasted_iota(jnp.int32, (8, 128), 1)

    for c in range(2):
        col_send[0, c] = load[0, c, :, 0:128].T[0:8]
        col_send[1, c] = load[0, c, :, cols - 128 : cols].T[120:128]

    fetches[1].wait()
    pl.semaphore_wait(barrier, len(WAYS))

    def copies(index):
        dx, dy = WAYS[index]
        width = slice(0, cols) if dy == 0 else (slice(0, 128) if dy < 0 else slice(cols - 128, cols))
        strip = slice(0, 8) if dx < 0 else slice(rows - 8, rows)
        third = 1 - dy
        if dx == 0:
            mat_src, mat_rows_at = slice(0, mat_rows), slice(0, mat_rows)
            src = col_send.at[0 if dy < 0 else 1]
            dst = col_halo.at[:, slice(0, 8) if dy < 0 else slice(120, 128), :]
        else:
            mat_src = slice(0, 8) if dx < 0 else slice(mat_rows - 8, mat_rows)
            mat_rows_at = slice(mat_rows, mat_rows + 8) if dx < 0 else slice(mat_rows + 8, mat_rows + 16)
            src = load.at[0, :, strip, width]
            if dy == 0:
                dst = row_halo.at[0 if dx < 0 else 1]
            else:
                dst = corner.at[0 if dx < 0 else 1, 0 if dy > 0 else 1]
        field = pltpu.make_async_remote_copy(
            src_ref=src, dst_ref=dst, send_sem=send_sem.at[2 * index], recv_sem=recv_sem.at[2 * index],
            device_id=at(dx, dy), device_id_type=MESH,
        )
        classes = pltpu.make_async_remote_copy(
            src_ref=material.at[0, mat_src, :], dst_ref=mat_halo.at[third, mat_rows_at, :],
            send_sem=send_sem.at[2 * index + 1], recv_sem=recv_sem.at[2 * index + 1],
            device_id=at(dx, dy), device_id_type=MESH,
        )
        return field, classes

    order = sorted(range(len(WAYS)), key=lambda i: -abs(WAYS[i][0]) - abs(WAYS[i][1]) - abs(WAYS[i][1]))
    for index in order:
        @pl.when(has[WAYS[index]])
        def _(index=index):
            for copy in copies(index):
                copy.start()

    for way in WAYS:
        pl.semaphore_signal(met.at[0], inc=1, device_id=at(*way), device_id_type=MESH)

    fetches[2].wait()
    mean = 0.0
    for k in range(CLASSES):
        mean = mean + (table[0, k] + 3.0 * table[1, k])
    inv_s = jnp.full((8, 128), (SPREAD / CLASSES) * mean, jnp.float32)
    quarter = 0.25 / inv_s

    def looked_up(classes):
        lam = jnp.zeros(classes.shape, jnp.float32)
        mu = jnp.zeros(classes.shape, jnp.float32)
        for k in range(CLASSES):
            hit = classes == k
            lam = jnp.where(hit, table[0, k], lam)
            mu = jnp.where(hit, table[1, k], mu)
        return lam, mu

    spread_row = lax.broadcasted_iota(jnp.int32, (mat_cols, cols), 0)
    spread_col = lax.broadcasted_iota(jnp.int32, (mat_cols, cols), 1)
    spread = (spread_row == spread_col // TILE).astype(jnp.float32)

    def widened(classes):
        lam, mu = looked_up(classes)
        both = jnp.concatenate([lam, mu], axis=0)
        wide = jnp.dot(both, spread, precision=lax.Precision.HIGHEST, preferred_element_type=jnp.float32)
        return wide[: classes.shape[0]], wide[classes.shape[0] :]

    def put_moduli(place, lam, mu):
        k, r = place
        small = quarter * mu
        moduli[0, k, r, :] = quarter * lam
        moduli[1, k, r, :] = small + small
        moduli[2, k, r, :] = small

    lam, mu = widened(material[0])
    for t in range(tiles):
        for k in range(planes):
            part = slice(128 * k, 128 * (k + 1))
            put_moduli(
                (k, slice(8 * t, 8 * t + 8)),
                jnp.broadcast_to(lam[t : t + 1, part], (8, 128)),
                jnp.broadcast_to(mu[t : t + 1, part], (8, 128)),
            )

    def own(t, acc):
        r = pl.ds(pl.multiple_of(8 * t, 8), 8)
        for c in range(2):
            for k in range(planes):
                value = load[0, c, r, 128 * k : 128 * (k + 1)]
                v[0, c, k, r, :] = value
                acc = acc + value * value
        return acc

    moments[0] = loop(tiles, own, jnp.zeros((8, 128), jnp.float32))

    last_lane, first_lane = lane == 127, lane == 0

    def shifted_left(parts):
        turned = [pltpu.roll(x, 127, 1) for x in parts]
        return [jnp.where(last_lane, turned[(k + 1) % len(parts)], turned[k]) for k in range(len(parts))]

    def shifted_right(parts):
        turned = [pltpu.roll(x, 1, 1) for x in parts]
        return [jnp.where(first_lane, turned[k - 1], turned[k]) for k in range(len(parts))]

    def first_shift(t, carry):
        r = pl.ds(pl.multiple_of(8 * t, 8), 8)
        for c in range(2):
            for k, value in enumerate(shifted_left([v[0, c, k, r, :] for k in range(planes)])[:-1]):
                vl[c, k, r, :] = value
        return carry

    loop(tiles, first_shift, 0)

    for index in range(len(WAYS)):
        dx, dy = WAYS[index]
        @pl.when(has[-dx, -dy])
        def _(index=index):
            for copy in copies(index):
                copy.wait_recv()

    low = sub < 4
    left_lanes = lane < 64
    inner_right = jnp.logical_and(lane < 4, has[0, 1])
    inner_left = jnp.logical_and(lane >= 124, has[0, -1])
    inner_lanes = jnp.logical_or(inner_right, inner_left)
    inner_below = jnp.logical_and(low, has[1, 0])
    inner_above = jnp.logical_and(sub >= 4, has[-1, 0])
    inner_subs = jnp.logical_or(inner_below, inner_above)
    inner_both = jnp.logical_and(inner_subs, inner_lanes)
    sub_mask = inner_subs.astype(jnp.float32)
    lane_mask = inner_lanes.astype(jnp.float32)
    halo = slice(rows, rows + 8)
    again = slice(rows + 8, rows + 16)
    for c in range(2):
        for k in range(planes):
            part = slice(128 * k, 128 * (k + 1))
            ring = jnp.where(low, row_halo[0, c, :, part], row_halo[1, c, :, part])
            v[0, c, k, halo, :] = jnp.where(inner_subs, ring, 0.0)
            v[0, c, k, again, :] = load[0, c, 0:8, part]
        beside = col_halo[c].T
        for t in range(tiles):
            value = jnp.where(inner_lanes, beside[8 * t : 8 * t + 8], 0.0)
            v[0, c, extra, 8 * t : 8 * t + 8, :] = value
            if t == 0:
                v[0, c, extra, again, :] = value
        below = jnp.where(left_lanes, corner[0, 1, c], corner[0, 0, c])
        above = jnp.where(left_lanes, corner[1, 1, c], corner[1, 0, c])
        v[0, c, extra, halo, :] = jnp.where(inner_both, jnp.where(low, below, above), 0.0)

    beyond = widened(mat_halo[1, mat_rows : mat_rows + 16, :])
    for k in range(planes):
        part = slice(128 * k, 128 * (k + 1))
        lam, mu = (
            jnp.where(
                inner_subs,
                jnp.where(low, jnp.broadcast_to(m[0:1, part], (8, 128)), jnp.broadcast_to(m[15:16, part], (8, 128))),
                0.0,
            )
            for m in beyond
        )
        put_moduli((k, halo), lam, mu)
    left, right = looked_up(mat_halo[0]), looked_up(mat_halo[2])
    for q in range(2):
        near = jnp.broadcast_to(right[q][:, 0:1], (mat_rows + 16, 128))
        far = jnp.broadcast_to(left[q][:, mat_cols - 1 : mat_cols], (mat_rows + 16, 128))
        wide_lane = lax.broadcasted_iota(jnp.int32, (mat_rows + 16, 128), 1)
        compact[q] = jnp.where(wide_lane < 64, near, far)
    for t in range(tiles):
        lam, mu = (
            jnp.where(inner_lanes, jnp.broadcast_to(compact[q, t : t + 1, :], (8, 128)), 0.0) for q in range(2)
        )
        put_moduli((extra, slice(8 * t, 8 * t + 8)), lam, mu)
    lam, mu = (
        jnp.where(
            inner_both,
            jnp.where(
                low,
                jnp.broadcast_to(compact[q, mat_rows : mat_rows + 1, :], (8, 128)),
                jnp.broadcast_to(compact[q, mat_rows + 15 : mat_rows + 16, :], (8, 128)),
            ),
            0.0,
        )
        for q in range(2)
    )
    put_moduli((extra, halo), lam, mu)

    def rest_shift(t, carry):
        r = pl.ds(pl.multiple_of(8 * t, 8), 8)
        for c in range(2):
            near, far, start = (v[0, c, k, r, :] for k in (planes - 1, extra, 0))
            for k, value in enumerate(shifted_left([near, far, start])[:-1]):
                vl[c, planes - 1 + k, r, :] = value
        return carry

    loop(tiles, rest_shift, 0)
    for c in range(2):
        for k, value in enumerate(shifted_left([v[0, c, k, halo, :] for k in range(SIDE)])):
            vl[c, k, halo, :] = value
        for k in range(SIDE):
            vl[c, k, again, :] = vl[c, k, 0:8, :]

    beyond_edge = jnp.logical_and(last_lane, jnp.logical_not(has[0, 1]))
    edge_mask = jnp.where(beyond_edge, 0.0, 1.0)
    moved_lanes = jnp.logical_or(
        jnp.logical_or(jnp.logical_and(lane < 3, has[0, 1]), last_lane),
        jnp.logical_and(jnp.logical_and(lane >= 123, lane < 127), has[0, -1]),
    )
    moved_mask = moved_lanes.astype(jnp.float32)

    pl.semaphore_wait(met.at[0], len(WAYS))
    for dx, dy in WAYS:
        pl.semaphore_signal(met.at[1], inc=1, device_id=at(2 * dx, 2 * dy), device_id_type=MESH)

    def level_step(level, carry):
        diag = jnp.where(level == 0, 0.0, DIAG)

        def stresses(t, carry):
            base = pl.multiple_of(8 * t, 8)
            r, rr = pl.ds(base, 8), pl.ds(base + 1, 8)
            for k in range(SIDE):
                d = []
                for c in range(2):
                    u = vl[c, k, rr, :] - v[level, c, k, r, :]
                    w = v[level, c, k, rr, :] - vl[c, k, r, :]
                    d.append((u + w, u - w))
                (dx0, dy0), (dx1, dy1) = d
                common = moduli[0, k, r, :] * (dx0 + dy1)
                twice = moduli[1, k, r, :]
                s = pl.ds(base + 8, 8)
                stress[0, k, s, :] = common + twice * dx0
                stress[1, k, s, :] = moduli[2, k, r, :] * (dy0 + dx1)
                stress[2, k, s, :] = common + twice * dy1
            return carry

        loop(tiles + 1, stresses, 0)
        for q in range(3):
            for k in range(SIDE):
                stress[q, k, 0:8, :] = stress[q, k, rows + 8 : rows + 16, :]

        def forces(base, acc, border):
            r, s, b = pl.ds(base, 8), pl.ds(base + 8, 8), pl.ds(base + 7, 8)
            plain, moved = ([], []), ([], [])
            for k in range(SIDE):
                xx, xy, yy = stress[0, k, s, :], stress[1, k, s, :], stress[2, k, s, :]
                xx_b, xy_b, yy_b = stress[0, k, b, :], stress[1, k, b, :], stress[2, k, b, :]
                dxx, sxy, dxy, syy = xx_b - xx, xy_b + xy, xy_b - xy, yy_b + yy
                plain[0].append(dxx - sxy)
                moved[0].append(dxx + sxy)
                plain[1].append(dxy - syy)
                moved[1].append(dxy + syy)
            for c in range(2):
                here = shifted_right(moved[c])
                there = shifted_left(plain[c])
                for k in range(SIDE):
                    old = v[level, c, k, r, :]
                    value = plain[c][k] + here[k] + diag * old
                    after = there[k] + moved[c][k] + diag * vl[c, k, r, :]
                    if border:
                        value, after = value * sub_mask, after * sub_mask
                    if k == extra:
                        value, after = value * lane_mask, after * moved_mask
                    elif k == extra - 1:
                        after = after * edge_mask
                    if k < extra and not border:
                        acc = (acc[0] + old * value, acc[1] + value * value)
                    v[level + 1, c, k, r, :] = value
                    vl[c, k, r, :] = after
            return acc

        zero = jnp.zeros((8, 128), jnp.float32)
        acc = loop(tiles, lambda t, acc: forces(pl.multiple_of(8 * t, 8), acc, False), (zero, zero))
        forces(rows, None, True)
        for c in range(2):
            for k in range(SIDE):
                v[level + 1, c, k, again, :] = v[level + 1, c, k, 0:8, :]
                vl[c, k, again, :] = vl[c, k, 0:8, :]
        moments[2 * level + 1] = acc[0]
        moments[2 * level + 2] = acc[1]
        return carry

    lax.fori_loop(0, LEVELS, level_step, 0)

    partial = jnp.sum(moments[0 : 2 * LEVELS], axis=1)
    partial = jnp.sum(partial, axis=1, keepdims=True)
    mine = jnp.sum(jnp.where(lane == sub, jnp.broadcast_to(partial, (8, 128)), 0.0), axis=0, keepdims=True)
    me = gx * ny + gy
    own_sum[0] = mine
    slots[me] = mine
    pl.semaphore_wait(met.at[1], len(WAYS))
    peers = [(a, b) for a in range(nx) for b in range(ny) if a or b]
    peers.sort(key=lambda w: -2 * min(w[1], ny - w[1]) - min(w[0], nx - w[0]))
    for way in peers:
        pltpu.make_async_remote_copy(
            src_ref=own_sum.at[0], dst_ref=slots.at[me], send_sem=sum_send.at[0], recv_sem=sum_recv.at[0],
            device_id=at(*way), device_id_type=MESH,
        ).start()
    everything = pltpu.make_async_remote_copy(
        src_ref=slots.at[0 : nx * ny - 1], dst_ref=slots.at[0 : nx * ny - 1],
        send_sem=sum_send.at[0], recv_sem=sum_recv.at[0], device_id=at(1, 0), device_id_type=MESH,
    )
    everything.wait_recv()
    mine = jnp.sum(slots[...], axis=0)

    g = [jnp.broadcast_to(mine[:, k : k + 1], (8, 128)) for k in range(2 * LEVELS)]
    m = [g[0], g[1]]
    for k in range(2, 2 * LEVELS):
        m.append(g[k] + DIAG * m[k - 1])
    sigma0 = jnp.full((8, 128), MASS, jnp.float32)
    sigma = sigma0 + (CENTRE / SPREAD) * inv_s
    shift = [sigma0] + [sigma] * (2 * LEVELS - 2)
    rho, phi = dict(enumerate(m)), dict(enumerate(m))
    one, nil = jnp.ones((8, 128), jnp.float32), jnp.zeros((8, 128), jnp.float32)
    r_of, p_of, x_of = [one] + [nil] * LEVELS, [one] + [nil] * LEVELS, [nil] * LEVELS
    for t in range(ITERS):
        psi = {l: phi[l + 1] * inv_s + shift[l] * phi[l] for l in range(t, 2 * LEVELS - 1 - t)}
        alpha = rho[t] / psi[t]
        for k in range(t + 1):
            x_of[k] = x_of[k] + alpha * p_of[k]
        ap = [
            (p_of[k - 1] * inv_s if k else nil) + (shift[k] * p_of[k] if k <= t else nil) for k in range(t + 2)
        ]
        for k in range(t + 2):
            r_of[k] = r_of[k] - alpha * ap[k]
        if t + 1 < ITERS:
            new = {l: rho[l] - alpha * psi[l] for l in range(t + 1, 2 * LEVELS - 1 - t)}
            beta = -(alpha * inv_s) * new[t + 1] / rho[t]
            phi = {l: new[l] + beta * phi[l] for l in new}
            rho = new
            for k in range(t + 2):
                p_of[k] = r_of[k] + beta * p_of[k]

    def combine(t, carry):
        r = pl.ds(pl.multiple_of(8 * t, 8), 8)
        for c in range(2):
            for k in range(planes):
                basis = [v[l, c, k, r, :] for l in range(LEVELS + 1)]
                part = slice(128 * k, 128 * (k + 1))
                x = x_of[0] * basis[0]
                for l in range(1, LEVELS):
                    x = x + x_of[l] * basis[l]
                res = r_of[0] * basis[0]
                for l in range(1, LEVELS + 1):
                    res = res + r_of[l] * basis[l]
                out_x[0, c, r, part] = x
                out_r[0, c, r, part] = res
        return carry

    loop(tiles, combine, 0)

    for index in range(len(WAYS)):
        @pl.when(has[WAYS[index]])
        def _(index=index):
            for copy in copies(index):
                copy.wait_send()
    everything.wait_send()


def on_device(nx, ny, load, material, lame_table):
    rows, cols = load.shape[2], load.shape[3]
    mat_rows, mat_cols = material.shape[1], material.shape[2]
    planes = cols // 128
    vmem = pl.BlockSpec(memory_space=pltpu.VMEM)
    f32 = jnp.float32
    return pl.pallas_call(
        functools.partial(kernel, nx, ny),
        out_shape=[jax.ShapeDtypeStruct(load.shape, f32)] * 2,
        in_specs=[pl.BlockSpec(memory_space=pltpu.HBM)] * 3,
        out_specs=[vmem, vmem],
        scratch_shapes=[
            pltpu.VMEM(load.shape, f32),
            pltpu.VMEM(material.shape, jnp.int32),
            pltpu.SMEM(lame_table.shape, f32),
            pltpu.VMEM((LEVELS + 1, 2, planes + 1, rows + 16, 128), f32),
            pltpu.VMEM((2, planes + 1, rows + 16, 128), f32),
            pltpu.VMEM((3, planes + 1, rows + 16, 128), f32),
            pltpu.VMEM((3, planes + 1, rows + 8, 128), f32),
            pltpu.VMEM((2, mat_rows + 16, 128), f32),
            pltpu.VMEM((2, 2, 8, cols), f32),
            pltpu.VMEM((2, 2, 8, 128), f32),
            pltpu.VMEM((2, 128, rows), f32),
            pltpu.VMEM((2, 2, 2, 8, 128), f32),
            pltpu.VMEM((3, mat_rows + 16, mat_cols), jnp.int32),
            pltpu.VMEM((nx * ny, 1, 128), f32),
            pltpu.VMEM((1, 1, 128), f32),
            pltpu.VMEM((2 * LEVELS + 1, 8, 128), f32),
            pltpu.SemaphoreType.DMA((3,)),
            pltpu.SemaphoreType.DMA((2 * len(WAYS),)),
            pltpu.SemaphoreType.DMA((2 * len(WAYS),)),
            pltpu.SemaphoreType.DMA((1,)),
            pltpu.SemaphoreType.DMA((1,)),
            pltpu.SemaphoreType.REGULAR((2,)),
        ],
        compiler_params=pltpu.CompilerParams(
            collective_id=0, has_side_effects=True, vmem_limit_bytes=24 * 1024 * 1024
        ),
    )(*(pltpu.with_memory_space_constraint(a, pltpu.HBM) for a in (load, material, lame_table)))


def solution(mesh):
    return jax.shard_map(
        functools.partial(on_device, mesh.shape["gx"], mesh.shape["gy"]),
        mesh=mesh,
        in_specs=(P("samp", None, "gx", "gy"), P("samp", "gx", "gy"), P()),
        out_specs=(P("samp", None, "gx", "gy"), P("samp", None, "gx", "gy")),
        check_vma=False,
    )
```

```python
import functools

import jax
import jax.numpy as jnp
from jax import lax
from jax.experimental import pallas as pl
from jax.experimental.pallas import tpu as pltpu
from jax.sharding import PartitionSpec as P

TILE = 8
CLASSES = 8
ITERS = 4
LEVELS = ITERS
MASS = 0.05
SPREAD = 1.5
CENTRE = 1.5
DIAG = -CENTRE / SPREAD
MESH = pl.DeviceIdType.MESH
WAYS = [(dx, dy) for dx in (-1, 0, 1) for dy in (-1, 0, 1) if (dx, dy) != (0, 0)]
SIDE = 5
PIECES = 4
DIAGONAL = [w for w in WAYS if w[0] and w[1]]


def loop(count, body, carry, unroll=None):
    return lax.fori_loop(0, count, body, carry, unroll=count if unroll is None else unroll)


def kernel(
    nx, ny, load_in, material_in, table_in, v, factors,
    load, material, table, vl, stress, moduli, compact, row_halo, col_send, col_halo, corner, mat_halo, slots,
    own_sum, moments, load_sem, send_sem, recv_sem, sum_send, sum_recv, met,
):
    rows, cols = load.shape[2], load.shape[3]
    tiles, planes = rows // 8, cols // 128
    mat_rows, mat_cols = material.shape[1], material.shape[2]
    extra = planes
    gx, gy = lax.axis_index("gx"), lax.axis_index("gy")
    has = {
        (-1, 0): gx > 0, (1, 0): gx < nx - 1, (0, -1): gy > 0, (0, 1): gy < ny - 1,
    }
    for dx, dy in DIAGONAL:
        has[dx, dy] = jnp.logical_and(has[dx, 0], has[0, dy])

    def at(dx, dy):
        return {"gx": lax.rem(gx + dx + nx, nx), "gy": lax.rem(gy + dy + ny, ny)}

    fetches = [
        pltpu.make_async_copy(load_in, load, load_sem.at[0]),
        pltpu.make_async_copy(material_in, material, load_sem.at[1]),
        pltpu.make_async_copy(table_in, table, load_sem.at[2]),
    ]
    fetches[0].start()
    barrier = pltpu.get_barrier_semaphore()
    for way in WAYS:
        pl.semaphore_signal(barrier, inc=1, device_id=at(*way), device_id_type=MESH)
    fetches[1].start()
    fetches[2].start()
    fetches[0].wait()

    sub = lax.broadcasted_iota(jnp.int32, (8, 128), 0)
    lane = lax.broadcasted_iota(jnp.int32, (8, 128), 1)

    for c in range(2):
        col_send[0, c] = load[0, c, :, 0:128].T[0:8]
        col_send[1, c] = load[0, c, :, cols - 128 : cols].T[120:128]

    fetches[1].wait()
    pl.semaphore_wait(barrier, len(WAYS))

    def copies(index):
        dx, dy = WAYS[index]
        width = slice(0, cols) if dy == 0 else (slice(0, 128) if dy < 0 else slice(cols - 128, cols))
        strip = slice(0, 8) if dx < 0 else slice(rows - 8, rows)
        third = 1 - dy
        if dx == 0:
            mat_src, mat_rows_at = slice(0, mat_rows), slice(0, mat_rows)
            src = col_send.at[0 if dy < 0 else 1]
            dst = col_halo.at[:, slice(0, 8) if dy < 0 else slice(120, 128), :]
        else:
            mat_src = slice(0, 8) if dx < 0 else slice(mat_rows - 8, mat_rows)
            mat_rows_at = slice(mat_rows, mat_rows + 8) if dx < 0 else slice(mat_rows + 8, mat_rows + 16)
            src = load.at[0, :, strip, width]
            if dy == 0:
                dst = row_halo.at[0 if dx < 0 else 1]
            else:
                dst = corner.at[0 if dx < 0 else 1, 0 if dy > 0 else 1]
        field = pltpu.make_async_remote_copy(
            src_ref=src, dst_ref=dst, send_sem=send_sem.at[2 * index], recv_sem=recv_sem.at[2 * index],
            device_id=at(dx, dy), device_id_type=MESH,
        )
        classes = pltpu.make_async_remote_copy(
            src_ref=material.at[0, mat_src, :], dst_ref=mat_halo.at[third, mat_rows_at, :],
            send_sem=send_sem.at[2 * index + 1], recv_sem=recv_sem.at[2 * index + 1],
            device_id=at(dx, dy), device_id_type=MESH,
        )
        return field, classes

    order = sorted(range(len(WAYS)), key=lambda i: -abs(WAYS[i][0]) - abs(WAYS[i][1]) - abs(WAYS[i][1]))
    for index in order:
        @pl.when(has[WAYS[index]])
        def _(index=index):
            for copy in copies(index):
                copy.start()

    for way in WAYS:
        pl.semaphore_signal(met.at[0], inc=1, device_id=at(*way), device_id_type=MESH)

    fetches[2].wait()
    mean = 0.0
    for k in range(CLASSES):
        mean = mean + (table[0, k] + 3.0 * table[1, k])
    inv_s = jnp.full((8, 128), (SPREAD / CLASSES) * mean, jnp.float32)
    quarter = 0.25 / inv_s

    def looked_up(classes):
        lam = jnp.zeros(classes.shape, jnp.float32)
        mu = jnp.zeros(classes.shape, jnp.float32)
        for k in range(CLASSES):
            hit = classes == k
            lam = jnp.where(hit, table[0, k], lam)
            mu = jnp.where(hit, table[1, k], mu)
        return lam, mu

    spread_row = lax.broadcasted_iota(jnp.int32, (mat_cols, cols), 0)
    spread_col = lax.broadcasted_iota(jnp.int32, (mat_cols, cols), 1)
    spread = (spread_row == spread_col // TILE).astype(jnp.float32)

    def widened(classes):
        lam, mu = looked_up(classes)
        both = jnp.concatenate([lam, mu], axis=0)
        wide = jnp.dot(both, spread, precision=lax.Precision.HIGHEST, preferred_element_type=jnp.float32)
        return wide[: classes.shape[0]], wide[classes.shape[0] :]

    def put_moduli(place, lam, mu):
        k, r = place
        small = quarter * mu
        moduli[0, k, r, :] = quarter * lam
        moduli[1, k, r, :] = small + small
        moduli[2, k, r, :] = small

    lam, mu = widened(material[0])
    for t in range(tiles):
        for k in range(planes):
            part = slice(128 * k, 128 * (k + 1))
            put_moduli(
                (k, slice(8 * t, 8 * t + 8)),
                jnp.broadcast_to(lam[t : t + 1, part], (8, 128)),
                jnp.broadcast_to(mu[t : t + 1, part], (8, 128)),
            )

    def own(t, acc):
        r = pl.ds(pl.multiple_of(8 * t, 8), 8)
        for c in range(2):
            for k in range(planes):
                value = load[0, c, r, 128 * k : 128 * (k + 1)]
                v[0, c, k, r, :] = value
                acc = acc + value * value
        return acc

    moments[0] = loop(tiles, own, jnp.zeros((8, 128), jnp.float32))

    last_lane, first_lane = lane == 127, lane == 0

    def shifted_left(parts):
        turned = [pltpu.roll(x, 127, 1) for x in parts]
        return [jnp.where(last_lane, turned[(k + 1) % len(parts)], turned[k]) for k in range(len(parts))]

    def shifted_right(parts):
        turned = [pltpu.roll(x, 1, 1) for x in parts]
        return [jnp.where(first_lane, turned[k - 1], turned[k]) for k in range(len(parts))]

    def first_shift(t, carry):
        r = pl.ds(pl.multiple_of(8 * t, 8), 8)
        for c in range(2):
            for k, value in enumerate(shifted_left([v[0, c, k, r, :] for k in range(planes)])[:-1]):
                vl[c, k, r, :] = value
        return carry

    loop(tiles, first_shift, 0)

    for index in range(len(WAYS)):
        dx, dy = WAYS[index]
        @pl.when(has[-dx, -dy])
        def _(index=index):
            for copy in copies(index):
                copy.wait_recv()

    low = sub < 4
    left_lanes = lane < 64
    inner_right = jnp.logical_and(lane < 4, has[0, 1])
    inner_left = jnp.logical_and(lane >= 124, has[0, -1])
    inner_lanes = jnp.logical_or(inner_right, inner_left)
    inner_below = jnp.logical_and(low, has[1, 0])
    inner_above = jnp.logical_and(sub >= 4, has[-1, 0])
    inner_subs = jnp.logical_or(inner_below, inner_above)
    inner_both = jnp.logical_and(inner_subs, inner_lanes)
    sub_mask = inner_subs.astype(jnp.float32)
    lane_mask = inner_lanes.astype(jnp.float32)
    halo = slice(rows, rows + 8)
    again = slice(rows + 8, rows + 16)
    for c in range(2):
        for k in range(planes):
            part = slice(128 * k, 128 * (k + 1))
            ring = jnp.where(low, row_halo[0, c, :, part], row_halo[1, c, :, part])
            v[0, c, k, halo, :] = jnp.where(inner_subs, ring, 0.0)
            v[0, c, k, again, :] = load[0, c, 0:8, part]
        beside = col_halo[c].T
        for t in range(tiles):
            value = jnp.where(inner_lanes, beside[8 * t : 8 * t + 8], 0.0)
            v[0, c, extra, 8 * t : 8 * t + 8, :] = value
            if t == 0:
                v[0, c, extra, again, :] = value
        below = jnp.where(left_lanes, corner[0, 1, c], corner[0, 0, c])
        above = jnp.where(left_lanes, corner[1, 1, c], corner[1, 0, c])
        v[0, c, extra, halo, :] = jnp.where(inner_both, jnp.where(low, below, above), 0.0)

    beyond = widened(mat_halo[1, mat_rows : mat_rows + 16, :])
    for k in range(planes):
        part = slice(128 * k, 128 * (k + 1))
        lam, mu = (
            jnp.where(
                inner_subs,
                jnp.where(low, jnp.broadcast_to(m[0:1, part], (8, 128)), jnp.broadcast_to(m[15:16, part], (8, 128))),
                0.0,
            )
            for m in beyond
        )
        put_moduli((k, halo), lam, mu)
    left, right = looked_up(mat_halo[0]), looked_up(mat_halo[2])
    for q in range(2):
        near = jnp.broadcast_to(right[q][:, 0:1], (mat_rows + 16, 128))
        far = jnp.broadcast_to(left[q][:, mat_cols - 1 : mat_cols], (mat_rows + 16, 128))
        wide_lane = lax.broadcasted_iota(jnp.int32, (mat_rows + 16, 128), 1)
        compact[q] = jnp.where(wide_lane < 64, near, far)
    for t in range(tiles):
        lam, mu = (
            jnp.where(inner_lanes, jnp.broadcast_to(compact[q, t : t + 1, :], (8, 128)), 0.0) for q in range(2)
        )
        put_moduli((extra, slice(8 * t, 8 * t + 8)), lam, mu)
    lam, mu = (
        jnp.where(
            inner_both,
            jnp.where(
                low,
                jnp.broadcast_to(compact[q, mat_rows : mat_rows + 1, :], (8, 128)),
                jnp.broadcast_to(compact[q, mat_rows + 15 : mat_rows + 16, :], (8, 128)),
            ),
            0.0,
        )
        for q in range(2)
    )
    put_moduli((extra, halo), lam, mu)

    def rest_shift(t, carry):
        r = pl.ds(pl.multiple_of(8 * t, 8), 8)
        for c in range(2):
            near, far, start = (v[0, c, k, r, :] for k in (planes - 1, extra, 0))
            for k, value in enumerate(shifted_left([near, far, start])[:-1]):
                vl[c, planes - 1 + k, r, :] = value
        return carry

    loop(tiles, rest_shift, 0)
    for c in range(2):
        for k, value in enumerate(shifted_left([v[0, c, k, halo, :] for k in range(SIDE)])):
            vl[c, k, halo, :] = value
        for k in range(SIDE):
            vl[c, k, again, :] = vl[c, k, 0:8, :]

    beyond_edge = jnp.logical_and(last_lane, jnp.logical_not(has[0, 1]))
    edge_mask = jnp.where(beyond_edge, 0.0, 1.0)
    moved_lanes = jnp.logical_or(
        jnp.logical_or(jnp.logical_and(lane < 3, has[0, 1]), last_lane),
        jnp.logical_and(jnp.logical_and(lane >= 123, lane < 127), has[0, -1]),
    )
    moved_mask = moved_lanes.astype(jnp.float32)

    pl.semaphore_wait(met.at[0], len(WAYS))
    for dx, dy in WAYS:
        pl.semaphore_signal(met.at[1], inc=1, device_id=at(2 * dx, 2 * dy), device_id_type=MESH)

    def stresses(level, tally):
        def body(t, energy):
            base = pl.multiple_of(8 * t, 8)
            r, rr = pl.ds(base, 8), pl.ds(base + 1, 8)
            for k in range(SIDE):
                d = []
                for c in range(2):
                    u = vl[c, k, rr, :] - v[level, c, k, r, :]
                    w = v[level, c, k, rr, :] - vl[c, k, r, :]
                    d.append((u + w, u - w))
                (dx0, dy0), (dx1, dy1) = d
                volume, shear = dx0 + dy1, dy0 + dx1
                common = moduli[0, k, r, :] * volume
                twice = moduli[1, k, r, :]
                xx, xy, yy = common + twice * dx0, moduli[2, k, r, :] * shear, common + twice * dy1
                if tally and k < extra:
                    energy = energy + (xx * dx0 + yy * dy1 + xy * shear)
                s = pl.ds(base + 8, 8)
                stress[0, k, s, :] = xx
                stress[1, k, s, :] = xy
                stress[2, k, s, :] = yy
            return energy

        energy = loop(tiles, body, jnp.zeros((8, 128), jnp.float32))
        tally = False
        body(tiles, energy)
        for q in range(3):
            for k in range(SIDE):
                stress[q, k, 0:8, :] = stress[q, k, rows + 8 : rows + 16, :]
        return energy

    def forces(level, base, acc, border, final):
        r, s, b = pl.ds(base, 8), pl.ds(base + 8, 8), pl.ds(base + 7, 8)
        plain, moved = ([], []), ([], [])
        for k in range(SIDE):
            xx, xy, yy = stress[0, k, s, :], stress[1, k, s, :], stress[2, k, s, :]
            xx_b, xy_b, yy_b = stress[0, k, b, :], stress[1, k, b, :], stress[2, k, b, :]
            dxx, sxy, dxy, syy = xx_b - xx, xy_b + xy, xy_b - xy, yy_b + yy
            plain[0].append(dxx - sxy)
            moved[0].append(dxx + sxy)
            plain[1].append(dxy - syy)
            moved[1].append(dxy + syy)
        for c in range(2):
            here = shifted_right(moved[c])
            there = None if final else shifted_left(plain[c])
            for k in range(planes if final else SIDE):
                old = v[level, c, k, r, :]
                value = plain[c][k] + here[k]
                if level:
                    value = value - old
                if final:
                    v[level + 1, c, k, r, :] = value
                    continue
                after = there[k] + moved[c][k]
                if level:
                    after = after - vl[c, k, r, :]
                if border:
                    value, after = value * sub_mask, after * sub_mask
                if k == extra:
                    value, after = value * lane_mask, after * moved_mask
                elif k == extra - 1:
                    after = after * edge_mask
                if k < extra and not border:
                    acc = (acc[0] + old * value, acc[1] + value * value)
                v[level + 1, c, k, r, :] = value
                vl[c, k, r, :] = after
        return acc

    zero = jnp.zeros((8, 128), jnp.float32)
    for level in range(LEVELS - 1):
        stresses(level, False)
        acc = loop(
            tiles,
            lambda t, acc, level=level: forces(level, pl.multiple_of(8 * t, 8), acc, False, False),
            (zero, zero),
        )
        forces(level, rows, None, True, False)
        for c in range(2):
            for k in range(SIDE):
                v[level + 1, c, k, again, :] = v[level + 1, c, k, 0:8, :]
                vl[c, k, again, :] = vl[c, k, 0:8, :]
        moments[2 * level + 1] = acc[0]
        moments[2 * level + 2] = acc[1]
    moments[2 * LEVELS - 1] = stresses(LEVELS - 1, True) + DIAG * moments[2 * LEVELS - 2]

    partial = jnp.sum(moments[0 : 2 * LEVELS], axis=1)
    partial = jnp.sum(partial, axis=1, keepdims=True)
    mine = jnp.sum(jnp.where(lane == sub, jnp.broadcast_to(partial, (8, 128)), 0.0), axis=0, keepdims=True)
    me = gx * ny + gy
    own_sum[0] = mine
    slots[me] = mine
    pl.semaphore_wait(met.at[1], len(WAYS))
    peers = [(a, b) for a in range(nx) for b in range(ny) if a or b]
    peers.sort(key=lambda w: -2 * min(w[1], ny - w[1]) - min(w[0], nx - w[0]))
    for way in peers:
        pltpu.make_async_remote_copy(
            src_ref=own_sum.at[0], dst_ref=slots.at[me], send_sem=sum_send.at[0], recv_sem=sum_recv.at[0],
            device_id=at(*way), device_id_type=MESH,
        ).start()
    everything = pltpu.make_async_remote_copy(
        src_ref=slots.at[0 : nx * ny - 1], dst_ref=slots.at[0 : nx * ny - 1],
        send_sem=sum_send.at[0], recv_sem=sum_recv.at[0], device_id=at(1, 0), device_id_type=MESH,
    )

    def final_forces(t, carry):
        forces(LEVELS - 1, pl.multiple_of(8 * t, 8), None, False, True)
        return carry

    loop(tiles, final_forces, 0)
    everything.wait_recv()
    mine = jnp.sum(slots[...], axis=0)

    g = [jnp.broadcast_to(mine[:, k : k + 1], (8, 128)) for k in range(2 * LEVELS)]
    m = [g[0], g[1]]
    for k in range(2, 2 * LEVELS):
        m.append(g[k] + DIAG * m[k - 1])
    sigma0 = jnp.full((8, 128), MASS, jnp.float32)
    sigma = sigma0 + (CENTRE / SPREAD) * inv_s
    shift = [sigma0] + [sigma] * (2 * LEVELS - 2)
    rho, phi = dict(enumerate(m)), dict(enumerate(m))
    one, nil = jnp.ones((8, 128), jnp.float32), jnp.zeros((8, 128), jnp.float32)
    r_of, p_of, x_of = [one] + [nil] * LEVELS, [one] + [nil] * LEVELS, [nil] * LEVELS
    for t in range(ITERS):
        psi = {l: phi[l + 1] * inv_s + shift[l] * phi[l] for l in range(t, 2 * LEVELS - 1 - t)}
        alpha = rho[t] / psi[t]
        for k in range(t + 1):
            x_of[k] = x_of[k] + alpha * p_of[k]
        ap = [
            (p_of[k - 1] * inv_s if k else nil) + (shift[k] * p_of[k] if k <= t else nil) for k in range(t + 2)
        ]
        for k in range(t + 2):
            r_of[k] = r_of[k] - alpha * ap[k]
        if t + 1 < ITERS:
            new = {l: rho[l] - alpha * psi[l] for l in range(t + 1, 2 * LEVELS - 1 - t)}
            beta = -(alpha * inv_s) * new[t + 1] / rho[t]
            phi = {l: new[l] + beta * phi[l] for l in new}
            rho = new
            for k in range(t + 2):
                p_of[k] = r_of[k] + beta * p_of[k]

    for k in range(LEVELS):
        factors[k] = x_of[k]
    for k in range(LEVELS + 1):
        factors[LEVELS + k] = r_of[k]

    for index in range(len(WAYS)):
        @pl.when(has[WAYS[index]])
        def _(index=index):
            for copy in copies(index):
                copy.wait_send()
    everything.wait_send()


def combine(v, factors, out_x, out_r, x_part, r_part, sems):
    rows, cols = out_x.shape[2], out_x.shape[3]
    planes = cols // 128
    x_of = [factors[k] for k in range(LEVELS)]
    r_of = [factors[LEVELS + k] for k in range(LEVELS + 1)]
    size = rows // PIECES
    copies = []
    for piece in range(PIECES):
        def body(t, carry):
            r = pl.ds(pl.multiple_of(piece * size + 8 * t, 8), 8)
            for c in range(2):
                for k in range(planes):
                    basis = [v[l, c, k, r, :] for l in range(LEVELS + 1)]
                    part = slice(128 * k, 128 * (k + 1))
                    x = x_of[0] * basis[0]
                    for l in range(1, LEVELS):
                        x = x + x_of[l] * basis[l]
                    res = r_of[0] * basis[0]
                    for l in range(1, LEVELS + 1):
                        res = res + r_of[l] * basis[l]
                    x_part[0, c, r, part] = x
                    r_part[0, c, r, part] = res
            return carry

        loop(size // 8, body, 0)
        here = pl.ds(piece * size, size)
        for i, (source, target) in enumerate(((x_part, out_x), (r_part, out_r))):
            copy = pltpu.make_async_copy(source.at[0, :, here, :], target.at[0, :, here, :], sems.at[i, piece])
            copy.start()
            copies.append(copy)
    for copy in copies:
        copy.wait()


def on_device(nx, ny, load, material, lame_table):
    rows, cols = load.shape[2], load.shape[3]
    mat_rows, mat_cols = material.shape[1], material.shape[2]
    planes = cols // 128
    vmem = pl.BlockSpec(memory_space=pltpu.VMEM)
    f32 = jnp.float32
    v, factors = pl.pallas_call(
        functools.partial(kernel, nx, ny),
        out_shape=[
            jax.ShapeDtypeStruct((LEVELS + 1, 2, planes + 1, rows + 16, 128), f32),
            jax.ShapeDtypeStruct((2 * LEVELS + 1, 8, 128), f32),
        ],
        in_specs=[pl.BlockSpec(memory_space=pltpu.HBM)] * 3,
        out_specs=[vmem, vmem],
        scratch_shapes=[
            pltpu.VMEM(load.shape, f32),
            pltpu.VMEM(material.shape, jnp.int32),
            pltpu.SMEM(lame_table.shape, f32),
            pltpu.VMEM((2, planes + 1, rows + 16, 128), f32),
            pltpu.VMEM((3, planes + 1, rows + 16, 128), f32),
            pltpu.VMEM((3, planes + 1, rows + 8, 128), f32),
            pltpu.VMEM((2, mat_rows + 16, 128), f32),
            pltpu.VMEM((2, 2, 8, cols), f32),
            pltpu.VMEM((2, 2, 8, 128), f32),
            pltpu.VMEM((2, 128, rows), f32),
            pltpu.VMEM((2, 2, 2, 8, 128), f32),
            pltpu.VMEM((3, mat_rows + 16, mat_cols), jnp.int32),
            pltpu.VMEM((nx * ny, 1, 128), f32),
            pltpu.VMEM((1, 1, 128), f32),
            pltpu.VMEM((2 * LEVELS, 8, 128), f32),
            pltpu.SemaphoreType.DMA((3,)),
            pltpu.SemaphoreType.DMA((2 * len(WAYS),)),
            pltpu.SemaphoreType.DMA((2 * len(WAYS),)),
            pltpu.SemaphoreType.DMA((1,)),
            pltpu.SemaphoreType.DMA((1,)),
            pltpu.SemaphoreType.REGULAR((2,)),
        ],
        compiler_params=pltpu.CompilerParams(
            collective_id=0, has_side_effects=True, vmem_limit_bytes=24 * 1024 * 1024
        ),
    )(*(pltpu.with_memory_space_constraint(a, pltpu.HBM) for a in (load, material, lame_table)))
    return pl.pallas_call(
        combine,
        out_shape=[jax.ShapeDtypeStruct(load.shape, f32)] * 2,
        in_specs=[vmem, vmem],
        out_specs=[pl.BlockSpec(memory_space=pltpu.HBM)] * 2,
        scratch_shapes=[
            pltpu.VMEM(load.shape, f32), pltpu.VMEM(load.shape, f32), pltpu.SemaphoreType.DMA((2, PIECES)),
        ],
        compiler_params=pltpu.CompilerParams(vmem_limit_bytes=24 * 1024 * 1024),
    )(v, factors)


def solution(mesh):
    return jax.shard_map(
        functools.partial(on_device, mesh.shape["gx"], mesh.shape["gy"]),
        mesh=mesh,
        in_specs=(P("samp", None, "gx", "gy"), P("samp", "gx", "gy"), P()),
        out_specs=(P("samp", None, "gx", "gy"), P("samp", None, "gx", "gy")),
        check_vma=False,
    )
```

```python
import functools

import jax
import jax.numpy as jnp
from jax import lax
from jax.experimental import pallas as pl
from jax.experimental.pallas import tpu as pltpu
from jax.sharding import PartitionSpec as P

TILE = 8
CLASSES = 8
ITERS = 4
LEVELS = ITERS
MASS = 0.05
SPREAD = 1.5
CENTRE = 1.5
DIAG = -CENTRE / SPREAD
MESH = pl.DeviceIdType.MESH
WAYS = [(dx, dy) for dx in (-1, 0, 1) for dy in (-1, 0, 1) if (dx, dy) != (0, 0)]
SIDE = 5
PIECES = 4
DIAGONAL = [w for w in WAYS if w[0] and w[1]]


def loop(count, body, carry, unroll=None):
    return lax.fori_loop(0, count, body, carry, unroll=count if unroll is None else unroll)


def kernel(
    nx, ny, load_in, material_in, table_in, v, factors,
    load, material, table, vl, stress, moduli, compact, row_halo, col_send, col_halo, corner, mat_halo, slots,
    own_sum, moments, load_sem, send_sem, recv_sem, sum_send, sum_recv, met,
):
    rows, cols = load.shape[2], load.shape[3]
    tiles, planes = rows // 8, cols // 128
    mat_rows, mat_cols = material.shape[1], material.shape[2]
    extra = planes
    gx, gy = lax.axis_index("gx"), lax.axis_index("gy")
    has = {
        (-1, 0): gx > 0, (1, 0): gx < nx - 1, (0, -1): gy > 0, (0, 1): gy < ny - 1,
    }
    for dx, dy in DIAGONAL:
        has[dx, dy] = jnp.logical_and(has[dx, 0], has[0, dy])

    def at(dx, dy):
        return {"gx": lax.rem(gx + dx + nx, nx), "gy": lax.rem(gy + dy + ny, ny)}

    fetches = [
        pltpu.make_async_copy(load_in, load, load_sem.at[0]),
        pltpu.make_async_copy(material_in, material, load_sem.at[1]),
        pltpu.make_async_copy(table_in, table, load_sem.at[2]),
    ]
    fetches[0].start()
    barrier = pltpu.get_barrier_semaphore()
    for way in WAYS:
        pl.semaphore_signal(barrier, inc=1, device_id=at(*way), device_id_type=MESH)
    fetches[1].start()
    fetches[2].start()
    fetches[0].wait()

    sub = lax.broadcasted_iota(jnp.int32, (8, 128), 0)
    lane = lax.broadcasted_iota(jnp.int32, (8, 128), 1)

    for c in range(2):
        col_send[0, c] = load[0, c, :, 0:128].T[0:8]
        col_send[1, c] = load[0, c, :, cols - 128 : cols].T[120:128]

    fetches[1].wait()
    pl.semaphore_wait(barrier, len(WAYS))

    def copies(index):
        dx, dy = WAYS[index]
        width = slice(0, cols) if dy == 0 else (slice(0, 128) if dy < 0 else slice(cols - 128, cols))
        strip = slice(0, 8) if dx < 0 else slice(rows - 8, rows)
        third = 1 - dy
        if dx == 0:
            mat_src, mat_rows_at = slice(0, mat_rows), slice(0, mat_rows)
            src = col_send.at[0 if dy < 0 else 1]
            dst = col_halo.at[:, slice(0, 8) if dy < 0 else slice(120, 128), :]
        else:
            mat_src = slice(0, 8) if dx < 0 else slice(mat_rows - 8, mat_rows)
            mat_rows_at = slice(mat_rows, mat_rows + 8) if dx < 0 else slice(mat_rows + 8, mat_rows + 16)
            src = load.at[0, :, strip, width]
            if dy == 0:
                dst = row_halo.at[0 if dx < 0 else 1]
            else:
                dst = corner.at[0 if dx < 0 else 1, 0 if dy > 0 else 1]
        field = pltpu.make_async_remote_copy(
            src_ref=src, dst_ref=dst, send_sem=send_sem.at[2 * index], recv_sem=recv_sem.at[2 * index],
            device_id=at(dx, dy), device_id_type=MESH,
        )
        classes = pltpu.make_async_remote_copy(
            src_ref=material.at[0, mat_src, :], dst_ref=mat_halo.at[third, mat_rows_at, :],
            send_sem=send_sem.at[2 * index + 1], recv_sem=recv_sem.at[2 * index + 1],
            device_id=at(dx, dy), device_id_type=MESH,
        )
        return field, classes

    order = sorted(range(len(WAYS)), key=lambda i: -abs(WAYS[i][0]) - abs(WAYS[i][1]) - abs(WAYS[i][1]))
    for index in order:
        @pl.when(has[WAYS[index]])
        def _(index=index):
            for copy in copies(index):
                copy.start()

    for way in WAYS:
        pl.semaphore_signal(met.at[0], inc=1, device_id=at(*way), device_id_type=MESH)

    fetches[2].wait()
    mean = 0.0
    for k in range(CLASSES):
        mean = mean + (table[0, k] + 3.0 * table[1, k])
    inv_s = jnp.full((8, 128), (SPREAD / CLASSES) * mean, jnp.float32)
    quarter = 0.25 / inv_s

    def looked_up(classes):
        lam = jnp.zeros(classes.shape, jnp.float32)
        mu = jnp.zeros(classes.shape, jnp.float32)
        for k in range(CLASSES):
            hit = classes == k
            lam = jnp.where(hit, table[0, k], lam)
            mu = jnp.where(hit, table[1, k], mu)
        return lam, mu

    spread_row = lax.broadcasted_iota(jnp.int32, (mat_cols, cols), 0)
    spread_col = lax.broadcasted_iota(jnp.int32, (mat_cols, cols), 1)
    spread = (spread_row == spread_col // TILE).astype(jnp.float32)

    def widened(classes):
        lam, mu = looked_up(classes)
        both = jnp.concatenate([lam, mu], axis=0)
        wide = jnp.dot(both, spread, precision=lax.Precision.HIGHEST, preferred_element_type=jnp.float32)
        return wide[: classes.shape[0]], wide[classes.shape[0] :]

    def put_moduli(place, lam, mu):
        k, r = place
        small = quarter * mu
        moduli[0, k, r, :] = quarter * lam
        moduli[1, k, r, :] = small + small
        moduli[2, k, r, :] = small

    lam, mu = widened(material[0])
    for t in range(tiles):
        for k in range(planes):
            part = slice(128 * k, 128 * (k + 1))
            put_moduli(
                (k, slice(8 * t, 8 * t + 8)),
                jnp.broadcast_to(lam[t : t + 1, part], (8, 128)),
                jnp.broadcast_to(mu[t : t + 1, part], (8, 128)),
            )

    def own(t, acc):
        r = pl.ds(pl.multiple_of(8 * t, 8), 8)
        for c in range(2):
            for k in range(planes):
                value = load[0, c, r, 128 * k : 128 * (k + 1)]
                v[0, c, k, r, :] = value
                acc = acc + value * value
        return acc

    moments[0] = loop(tiles, own, jnp.zeros((8, 128), jnp.float32))

    last_lane, first_lane = lane == 127, lane == 0

    def shifted_left(parts):
        turned = [pltpu.roll(x, 127, 1) for x in parts]
        return [jnp.where(last_lane, turned[(k + 1) % len(parts)], turned[k]) for k in range(len(parts))]

    def first_shift(t, carry):
        r = pl.ds(pl.multiple_of(8 * t, 8), 8)
        for c in range(2):
            for k, value in enumerate(shifted_left([v[0, c, k, r, :] for k in range(planes)])):
                vl[c, k, r, :] = value
        return carry

    loop(tiles, first_shift, 0)

    low = sub < 4
    left_lanes = lane < 64
    inner_right = jnp.logical_and(lane < 4, has[0, 1])
    inner_left = jnp.logical_and(lane >= 124, has[0, -1])
    inner_lanes = jnp.logical_or(inner_right, inner_left)
    inner_below = jnp.logical_and(low, has[1, 0])
    inner_above = jnp.logical_and(sub >= 4, has[-1, 0])
    inner_subs = jnp.logical_or(inner_below, inner_above)
    inner_both = jnp.logical_and(inner_subs, inner_lanes)
    sub_mask = inner_subs.astype(jnp.float32)
    lane_mask = inner_lanes.astype(jnp.float32)
    beyond_edge = jnp.logical_and(last_lane, jnp.logical_not(has[0, 1]))
    edge_mask = jnp.where(beyond_edge, 0.0, 1.0)
    moved_lanes = jnp.logical_or(
        jnp.logical_or(jnp.logical_and(lane < 3, has[0, 1]), last_lane),
        jnp.logical_and(jnp.logical_and(lane >= 123, lane < 127), has[0, -1]),
    )
    moved_mask = moved_lanes.astype(jnp.float32)
    halo = slice(rows, rows + 8)
    again = slice(rows + 8, rows + 16)
    zero = jnp.zeros((8, 128), jnp.float32)
    everywhere = tuple(range(SIDE))

    def stresses(level, base, where, energy=None):
        r, rr, s = pl.ds(base, 8), pl.ds(base + 1, 8), pl.ds(base + 8, 8)
        for k in where:
            d = []
            for c in range(2):
                u = vl[c, k, rr, :] - v[level, c, k, r, :]
                w = v[level, c, k, rr, :] - vl[c, k, r, :]
                d.append((u + w, u - w))
            (dx0, dy0), (dx1, dy1) = d
            volume, shear = dx0 + dy1, dy0 + dx1
            common = moduli[0, k, r, :] * volume
            twice = moduli[1, k, r, :]
            xx, xy, yy = common + twice * dx0, moduli[2, k, r, :] * shear, common + twice * dy1
            if energy is not None and k < extra:
                energy = energy + (xx * dx0 + yy * dy1 + xy * shear)
            stress[0, k, s, :] = xx
            stress[1, k, s, :] = xy
            stress[2, k, s, :] = yy
        return energy

    def row_before():
        for q in range(3):
            for k in range(SIDE):
                stress[q, k, 0:8, :] = stress[q, k, rows + 8 : rows + 16, :]

    def forces(level, base, acc, where, border=False, final=False):
        r, s, b = pl.ds(base, 8), pl.ds(base + 8, 8), pl.ds(base + 7, 8)
        before = {(k - 1) % SIDE for k in where}
        behind = set() if final else {(k + 1) % SIDE for k in where}
        plain, moved = ({}, {}), ({}, {})
        for k in sorted(before | behind | set(where)):
            xx, xy, yy = stress[0, k, s, :], stress[1, k, s, :], stress[2, k, s, :]
            xx_b, xy_b, yy_b = stress[0, k, b, :], stress[1, k, b, :], stress[2, k, b, :]
            dxx, sxy, dxy, syy = xx_b - xx, xy_b + xy, xy_b - xy, yy_b + yy
            if k in where or k in behind:
                plain[0][k] = dxx - sxy
                plain[1][k] = dxy - syy
            if k in where or k in before:
                moved[0][k] = dxx + sxy
                moved[1][k] = dxy + syy
        for c in range(2):
            turned = {k: pltpu.roll(x, 1, 1) for k, x in moved[c].items()}
            returned = {} if final else {k: pltpu.roll(x, 127, 1) for k, x in plain[c].items()}
            for k in where:
                old = v[level, c, k, r, :]
                value = plain[c][k] + jnp.where(first_lane, turned[(k - 1) % SIDE], turned[k])
                if level:
                    value = value - old
                if final:
                    v[level + 1, c, k, r, :] = value
                    continue
                after = jnp.where(last_lane, returned[(k + 1) % SIDE], returned[k]) + moved[c][k]
                if level:
                    after = after - vl[c, k, r, :]
                if border:
                    value, after = value * sub_mask, after * sub_mask
                if k == extra:
                    value, after = value * lane_mask, after * moved_mask
                elif k == extra - 1:
                    after = after * edge_mask
                if k < extra and not border:
                    acc = (acc[0] + old * value, acc[1] + value * value)
                v[level + 1, c, k, r, :] = value
                vl[c, k, r, :] = after
        return acc

    def vector_done(level, acc):
        for c in range(2):
            for k in range(SIDE):
                v[level + 1, c, k, again, :] = v[level + 1, c, k, 0:8, :]
                vl[c, k, again, :] = vl[c, k, 0:8, :]
        moments[2 * level + 1] = acc[0]
        moments[2 * level + 2] = acc[1]

    def rows_from(t):
        return pl.multiple_of(8 * t, 8)

    inside = tuple(range(1, planes - 1))
    outside = tuple(k for k in everywhere if k not in inside)

    def stress_inside(t, carry):
        stresses(0, rows_from(t), range(planes))
        return carry

    loop(tiles - 1, stress_inside, 0)
    acc = loop(tiles - 2, lambda t, acc: forces(0, rows_from(t + 1), acc, inside), (zero, zero))

    pl.semaphore_wait(met.at[0], len(WAYS))
    for dx, dy in WAYS:
        pl.semaphore_signal(met.at[1], inc=1, device_id=at(2 * dx, 2 * dy), device_id_type=MESH)

    def arrived(ways):
        for index in range(len(WAYS)):
            dx, dy = WAYS[index]
            if (dx, dy) in ways:
                @pl.when(has[-dx, -dy])
                def _(index=index):
                    for copy in copies(index):
                        copy.wait_recv()

    def beside_moduli(part):
        left, right = looked_up(mat_halo[0, part, :]), looked_up(mat_halo[2, part, :])
        size = part.stop - part.start
        wide_lane = lax.broadcasted_iota(jnp.int32, (size, 128), 1)
        for q in range(2):
            near = jnp.broadcast_to(right[q][:, 0:1], (size, 128))
            far = jnp.broadcast_to(left[q][:, mat_cols - 1 : mat_cols], (size, 128))
            compact[q, part, :] = jnp.where(wide_lane < 64, near, far)

    arrived([(0, -1), (0, 1)])
    for c in range(2):
        beside = col_halo[c].T
        for t in range(tiles):
            v[0, c, extra, 8 * t : 8 * t + 8, :] = jnp.where(inner_lanes, beside[8 * t : 8 * t + 8], 0.0)
    beside_moduli(slice(0, mat_rows))
    for t in range(tiles):
        lam, mu = (
            jnp.where(inner_lanes, jnp.broadcast_to(compact[q, t : t + 1, :], (8, 128)), 0.0) for q in range(2)
        )
        put_moduli((extra, slice(8 * t, 8 * t + 8)), lam, mu)

    def rest_shift(t, carry):
        r = pl.ds(rows_from(t), 8)
        for c in range(2):
            near, far, start = (v[0, c, k, r, :] for k in (planes - 1, extra, 0))
            for k, value in enumerate(shifted_left([near, far, start])[:-1]):
                vl[c, planes - 1 + k, r, :] = value
        return carry

    loop(tiles, rest_shift, 0)

    def stress_outside(t, carry):
        stresses(0, rows_from(t), (planes - 1, extra))
        return carry

    loop(tiles - 1, stress_outside, 0)
    acc = loop(tiles - 2, lambda t, acc: forces(0, rows_from(t + 1), acc, outside), acc)

    arrived([way for way in WAYS if way[0]])
    for c in range(2):
        for k in range(planes):
            part = slice(128 * k, 128 * (k + 1))
            ring = jnp.where(low, row_halo[0, c, :, part], row_halo[1, c, :, part])
            v[0, c, k, halo, :] = jnp.where(inner_subs, ring, 0.0)
        below = jnp.where(left_lanes, corner[0, 1, c], corner[0, 0, c])
        above = jnp.where(left_lanes, corner[1, 1, c], corner[1, 0, c])
        v[0, c, extra, halo, :] = jnp.where(inner_both, jnp.where(low, below, above), 0.0)
        for k in range(SIDE):
            v[0, c, k, again, :] = v[0, c, k, 0:8, :]
    beyond = widened(mat_halo[1, mat_rows : mat_rows + 16, :])
    for k in range(planes):
        part = slice(128 * k, 128 * (k + 1))
        lam, mu = (
            jnp.where(
                inner_subs,
                jnp.where(low, jnp.broadcast_to(m[0:1, part], (8, 128)), jnp.broadcast_to(m[15:16, part], (8, 128))),
                0.0,
            )
            for m in beyond
        )
        put_moduli((k, halo), lam, mu)
    beside_moduli(slice(mat_rows, mat_rows + 16))
    lam, mu = (
        jnp.where(
            inner_both,
            jnp.where(
                low,
                jnp.broadcast_to(compact[q, mat_rows : mat_rows + 1, :], (8, 128)),
                jnp.broadcast_to(compact[q, mat_rows + 15 : mat_rows + 16, :], (8, 128)),
            ),
            0.0,
        )
        for q in range(2)
    )
    put_moduli((extra, halo), lam, mu)
    for c in range(2):
        for k, value in enumerate(shifted_left([v[0, c, k, halo, :] for k in range(SIDE)])):
            vl[c, k, halo, :] = value
        for k in range(SIDE):
            vl[c, k, again, :] = vl[c, k, 0:8, :]
    stresses(0, rows - 8, everywhere)
    stresses(0, rows, everywhere)
    row_before()
    acc = forces(0, 0, acc, everywhere)
    acc = forces(0, rows - 8, acc, everywhere)
    forces(0, rows, None, everywhere, border=True)
    vector_done(0, acc)

    for level in range(1, LEVELS - 1):
        def stress_step(t, carry, level=level):
            stresses(level, rows_from(t), everywhere)
            return carry

        loop(tiles + 1, stress_step, 0)
        row_before()
        acc = loop(
            tiles, lambda t, acc, level=level: forces(level, rows_from(t), acc, everywhere), (zero, zero)
        )
        forces(level, rows, None, everywhere, border=True)
        vector_done(level, acc)
    last = LEVELS - 1
    energy = loop(tiles, lambda t, energy: stresses(last, rows_from(t), everywhere, energy), zero)
    stresses(last, rows, everywhere)
    row_before()
    moments[2 * LEVELS - 1] = energy + DIAG * moments[2 * LEVELS - 2]

    partial = jnp.sum(moments[0 : 2 * LEVELS], axis=1)
    partial = jnp.sum(partial, axis=1, keepdims=True)
    mine = jnp.sum(jnp.where(lane == sub, jnp.broadcast_to(partial, (8, 128)), 0.0), axis=0, keepdims=True)
    me = gx * ny + gy
    own_sum[0] = mine
    slots[me] = mine
    pl.semaphore_wait(met.at[1], len(WAYS))
    peers = [(a, b) for a in range(nx) for b in range(ny) if a or b]
    peers.sort(key=lambda w: -2 * min(w[1], ny - w[1]) - min(w[0], nx - w[0]))
    for way in peers:
        pltpu.make_async_remote_copy(
            src_ref=own_sum.at[0], dst_ref=slots.at[me], send_sem=sum_send.at[0], recv_sem=sum_recv.at[0],
            device_id=at(*way), device_id_type=MESH,
        ).start()
    everything = pltpu.make_async_remote_copy(
        src_ref=slots.at[0 : nx * ny - 1], dst_ref=slots.at[0 : nx * ny - 1],
        send_sem=sum_send.at[0], recv_sem=sum_recv.at[0], device_id=at(1, 0), device_id_type=MESH,
    )

    def final_forces(t, carry):
        forces(last, rows_from(t), None, range(planes), final=True)
        return carry

    loop(tiles, final_forces, 0)
    everything.wait_recv()
    mine = jnp.sum(slots[...], axis=0)

    g = [jnp.broadcast_to(mine[:, k : k + 1], (8, 128)) for k in range(2 * LEVELS)]
    m = [g[0], g[1]]
    for k in range(2, 2 * LEVELS):
        m.append(g[k] + DIAG * m[k - 1])
    sigma0 = jnp.full((8, 128), MASS, jnp.float32)
    sigma = sigma0 + (CENTRE / SPREAD) * inv_s
    shift = [sigma0] + [sigma] * (2 * LEVELS - 2)
    rho, phi = dict(enumerate(m)), dict(enumerate(m))
    one, nil = jnp.ones((8, 128), jnp.float32), jnp.zeros((8, 128), jnp.float32)
    r_of, p_of, x_of = [one] + [nil] * LEVELS, [one] + [nil] * LEVELS, [nil] * LEVELS
    for t in range(ITERS):
        psi = {l: phi[l + 1] * inv_s + shift[l] * phi[l] for l in range(t, 2 * LEVELS - 1 - t)}
        alpha = rho[t] / psi[t]
        for k in range(t + 1):
            x_of[k] = x_of[k] + alpha * p_of[k]
        ap = [
            (p_of[k - 1] * inv_s if k else nil) + (shift[k] * p_of[k] if k <= t else nil) for k in range(t + 2)
        ]
        for k in range(t + 2):
            r_of[k] = r_of[k] - alpha * ap[k]
        if t + 1 < ITERS:
            new = {l: rho[l] - alpha * psi[l] for l in range(t + 1, 2 * LEVELS - 1 - t)}
            beta = -(alpha * inv_s) * new[t + 1] / rho[t]
            phi = {l: new[l] + beta * phi[l] for l in new}
            rho = new
            for k in range(t + 2):
                p_of[k] = r_of[k] + beta * p_of[k]

    for k in range(LEVELS):
        factors[k] = x_of[k]
    for k in range(LEVELS + 1):
        factors[LEVELS + k] = r_of[k]

    for index in range(len(WAYS)):
        @pl.when(has[WAYS[index]])
        def _(index=index):
            for copy in copies(index):
                copy.wait_send()
    everything.wait_send()


def combine(v, factors, out_x, out_r, x_part, r_part, sems):
    rows, cols = out_x.shape[2], out_x.shape[3]
    planes = cols // 128
    x_of = [factors[k] for k in range(LEVELS)]
    r_of = [factors[LEVELS + k] for k in range(LEVELS + 1)]
    size = rows // PIECES
    copies = []
    for piece in range(PIECES):
        def body(t, carry):
            r = pl.ds(pl.multiple_of(piece * size + 8 * t, 8), 8)
            for c in range(2):
                for k in range(planes):
                    basis = [v[l, c, k, r, :] for l in range(LEVELS + 1)]
                    part = slice(128 * k, 128 * (k + 1))
                    x = x_of[0] * basis[0]
                    for l in range(1, LEVELS):
                        x = x + x_of[l] * basis[l]
                    res = r_of[0] * basis[0]
                    for l in range(1, LEVELS + 1):
                        res = res + r_of[l] * basis[l]
                    x_part[0, c, r, part] = x
                    r_part[0, c, r, part] = res
            return carry

        loop(size // 8, body, 0)
        here = pl.ds(piece * size, size)
        for i, (source, target) in enumerate(((x_part, out_x), (r_part, out_r))):
            copy = pltpu.make_async_copy(source.at[0, :, here, :], target.at[0, :, here, :], sems.at[i, piece])
            copy.start()
            copies.append(copy)
    for copy in copies:
        copy.wait()


def on_device(nx, ny, load, material, lame_table):
    rows, cols = load.shape[2], load.shape[3]
    mat_rows, mat_cols = material.shape[1], material.shape[2]
    planes = cols // 128
    vmem = pl.BlockSpec(memory_space=pltpu.VMEM)
    f32 = jnp.float32
    v, factors = pl.pallas_call(
        functools.partial(kernel, nx, ny),
        out_shape=[
            jax.ShapeDtypeStruct((LEVELS + 1, 2, planes + 1, rows + 16, 128), f32),
            jax.ShapeDtypeStruct((2 * LEVELS + 1, 8, 128), f32),
        ],
        in_specs=[pl.BlockSpec(memory_space=pltpu.HBM)] * 3,
        out_specs=[vmem, vmem],
        scratch_shapes=[
            pltpu.VMEM(load.shape, f32),
            pltpu.VMEM(material.shape, jnp.int32),
            pltpu.SMEM(lame_table.shape, f32),
            pltpu.VMEM((2, planes + 1, rows + 16, 128), f32),
            pltpu.VMEM((3, planes + 1, rows + 16, 128), f32),
            pltpu.VMEM((3, planes + 1, rows + 8, 128), f32),
            pltpu.VMEM((2, mat_rows + 16, 128), f32),
            pltpu.VMEM((2, 2, 8, cols), f32),
            pltpu.VMEM((2, 2, 8, 128), f32),
            pltpu.VMEM((2, 128, rows), f32),
            pltpu.VMEM((2, 2, 2, 8, 128), f32),
            pltpu.VMEM((3, mat_rows + 16, mat_cols), jnp.int32),
            pltpu.VMEM((nx * ny, 1, 128), f32),
            pltpu.VMEM((1, 1, 128), f32),
            pltpu.VMEM((2 * LEVELS, 8, 128), f32),
            pltpu.SemaphoreType.DMA((3,)),
            pltpu.SemaphoreType.DMA((2 * len(WAYS),)),
            pltpu.SemaphoreType.DMA((2 * len(WAYS),)),
            pltpu.SemaphoreType.DMA((1,)),
            pltpu.SemaphoreType.DMA((1,)),
            pltpu.SemaphoreType.REGULAR((2,)),
        ],
        compiler_params=pltpu.CompilerParams(
            collective_id=0, has_side_effects=True, vmem_limit_bytes=24 * 1024 * 1024
        ),
    )(*(pltpu.with_memory_space_constraint(a, pltpu.HBM) for a in (load, material, lame_table)))
    return pl.pallas_call(
        combine,
        out_shape=[jax.ShapeDtypeStruct(load.shape, f32)] * 2,
        in_specs=[vmem, vmem],
        out_specs=[pl.BlockSpec(memory_space=pltpu.HBM)] * 2,
        scratch_shapes=[
            pltpu.VMEM(load.shape, f32), pltpu.VMEM(load.shape, f32), pltpu.SemaphoreType.DMA((2, PIECES)),
        ],
        compiler_params=pltpu.CompilerParams(vmem_limit_bytes=24 * 1024 * 1024),
    )(v, factors)


def solution(mesh):
    return jax.shard_map(
        functools.partial(on_device, mesh.shape["gx"], mesh.shape["gy"]),
        mesh=mesh,
        in_specs=(P("samp", None, "gx", "gy"), P("samp", "gx", "gy"), P()),
        out_specs=(P("samp", None, "gx", "gy"), P("samp", None, "gx", "gy")),
        check_vma=False,
    )
```

```python
import functools

import jax
import jax.numpy as jnp
from jax import lax
from jax.experimental import pallas as pl
from jax.experimental.pallas import tpu as pltpu
from jax.sharding import PartitionSpec as P

TILE = 8
CLASSES = 8
ITERS = 4
LEVELS = ITERS
MASS = 0.05
SPREAD = 1.5
CENTRE = 1.5
DIAG = -CENTRE / SPREAD
MESH = pl.DeviceIdType.MESH
WAYS = [(dx, dy) for dx in (-1, 0, 1) for dy in (-1, 0, 1) if (dx, dy) != (0, 0)]
SIDE = 5
PIECES = 4
DIAGONAL = [w for w in WAYS if w[0] and w[1]]


def loop(count, body, carry, unroll=None):
    return lax.fori_loop(0, count, body, carry, unroll=count if unroll is None else unroll)


def kernel(
    nx, ny, load_in, material_in, table_in, v, factors,
    load, material, table, vl, stress, moduli, compact, row_halo, col_send, col_halo, corner, mat_halo, slots,
    own_sum, moments, load_sem, send_sem, recv_sem, sum_send, sum_recv, met,
):
    rows, cols = load.shape[2], load.shape[3]
    tiles, planes = rows // 8, cols // 128
    mat_rows, mat_cols = material.shape[1], material.shape[2]
    extra = planes
    gx, gy = lax.axis_index("gx"), lax.axis_index("gy")
    has = {
        (-1, 0): gx > 0, (1, 0): gx < nx - 1, (0, -1): gy > 0, (0, 1): gy < ny - 1,
    }
    for dx, dy in DIAGONAL:
        has[dx, dy] = jnp.logical_and(has[dx, 0], has[0, dy])

    def at(dx, dy):
        return {"gx": lax.rem(gx + dx + nx, nx), "gy": lax.rem(gy + dy + ny, ny)}

    fetches = [
        pltpu.make_async_copy(load_in, load, load_sem.at[0]),
        pltpu.make_async_copy(material_in, material, load_sem.at[1]),
        pltpu.make_async_copy(table_in, table, load_sem.at[2]),
    ]
    fetches[0].start()
    barrier = pltpu.get_barrier_semaphore()
    for way in WAYS:
        pl.semaphore_signal(barrier, inc=1, device_id=at(*way), device_id_type=MESH)
    fetches[1].start()
    fetches[2].start()
    fetches[0].wait()

    sub = lax.broadcasted_iota(jnp.int32, (8, 128), 0)
    lane = lax.broadcasted_iota(jnp.int32, (8, 128), 1)

    for c in range(2):
        col_send[0, c] = load[0, c, :, 0:128].T[0:8]
        col_send[1, c] = load[0, c, :, cols - 128 : cols].T[120:128]

    fetches[1].wait()
    pl.semaphore_wait(barrier, len(WAYS))

    def copies(index):
        dx, dy = WAYS[index]
        width = slice(0, cols) if dy == 0 else (slice(0, 128) if dy < 0 else slice(cols - 128, cols))
        strip = slice(0, 8) if dx < 0 else slice(rows - 8, rows)
        third = 1 - dy
        if dx == 0:
            mat_src, mat_rows_at = slice(0, mat_rows), slice(0, mat_rows)
            src = col_send.at[0 if dy < 0 else 1]
            dst = col_halo.at[:, slice(0, 8) if dy < 0 else slice(120, 128), :]
        else:
            mat_src = slice(0, 8) if dx < 0 else slice(mat_rows - 8, mat_rows)
            mat_rows_at = slice(mat_rows, mat_rows + 8) if dx < 0 else slice(mat_rows + 8, mat_rows + 16)
            src = load.at[0, :, strip, width]
            if dy == 0:
                dst = row_halo.at[0 if dx < 0 else 1]
            else:
                dst = corner.at[0 if dx < 0 else 1, 0 if dy > 0 else 1]
        field = pltpu.make_async_remote_copy(
            src_ref=src, dst_ref=dst, send_sem=send_sem.at[2 * index], recv_sem=recv_sem.at[2 * index],
            device_id=at(dx, dy), device_id_type=MESH,
        )
        classes = pltpu.make_async_remote_copy(
            src_ref=material.at[0, mat_src, :], dst_ref=mat_halo.at[third, mat_rows_at, :],
            send_sem=send_sem.at[2 * index + 1], recv_sem=recv_sem.at[2 * index + 1],
            device_id=at(dx, dy), device_id_type=MESH,
        )
        return field, classes

    order = sorted(range(len(WAYS)), key=lambda i: -abs(WAYS[i][0]) - abs(WAYS[i][1]) - abs(WAYS[i][1]))
    for index in order:
        @pl.when(has[WAYS[index]])
        def _(index=index):
            for copy in copies(index):
                copy.start()

    for way in WAYS:
        pl.semaphore_signal(met.at[0], inc=1, device_id=at(*way), device_id_type=MESH)

    fetches[2].wait()
    mean = 0.0
    for k in range(CLASSES):
        mean = mean + (table[0, k] + 3.0 * table[1, k])
    inv_s = jnp.full((8, 128), (SPREAD / CLASSES) * mean, jnp.float32)
    quarter = 0.25 / inv_s

    def looked_up(classes):
        lam = jnp.zeros(classes.shape, jnp.float32)
        mu = jnp.zeros(classes.shape, jnp.float32)
        for k in range(CLASSES):
            hit = classes == k
            lam = jnp.where(hit, table[0, k], lam)
            mu = jnp.where(hit, table[1, k], mu)
        return lam, mu

    spread_row = lax.broadcasted_iota(jnp.int32, (mat_cols, cols), 0)
    spread_col = lax.broadcasted_iota(jnp.int32, (mat_cols, cols), 1)
    spread = (spread_row == spread_col // TILE).astype(jnp.float32)

    def widened(classes):
        lam, mu = looked_up(classes)
        both = jnp.concatenate([lam, mu], axis=0)
        wide = jnp.dot(both, spread, precision=lax.Precision.HIGHEST, preferred_element_type=jnp.float32)
        return wide[: classes.shape[0]], wide[classes.shape[0] :]

    def put_moduli(place, lam, mu):
        k, r = place
        small = quarter * mu
        moduli[0, k, r, :] = quarter * lam
        moduli[1, k, r, :] = small + small
        moduli[2, k, r, :] = small

    lam, mu = widened(material[0])
    for t in range(tiles):
        for k in range(planes):
            part = slice(128 * k, 128 * (k + 1))
            put_moduli(
                (k, slice(8 * t, 8 * t + 8)),
                jnp.broadcast_to(lam[t : t + 1, part], (8, 128)),
                jnp.broadcast_to(mu[t : t + 1, part], (8, 128)),
            )

    def own(t, acc):
        r = pl.ds(pl.multiple_of(8 * t, 8), 8)
        for c in range(2):
            for k in range(planes):
                value = load[0, c, r, 128 * k : 128 * (k + 1)]
                v[0, c, k, r, :] = value
                acc = acc + value * value
        return acc

    moments[0] = loop(tiles, own, jnp.zeros((8, 128), jnp.float32))

    last_lane, first_lane = lane == 127, lane == 0

    def shifted_left(parts):
        turned = [pltpu.roll(x, 127, 1) for x in parts]
        return [jnp.where(last_lane, turned[(k + 1) % len(parts)], turned[k]) for k in range(len(parts))]

    def first_shift(t, carry):
        r = pl.ds(pl.multiple_of(8 * t, 8), 8)
        for c in range(2):
            for k, value in enumerate(shifted_left([v[0, c, k, r, :] for k in range(planes)])):
                vl[0, c, k, r, :] = value
        return carry

    loop(tiles, first_shift, 0)

    low = sub < 4
    left_lanes = lane < 64
    inner_right = jnp.logical_and(lane < 4, has[0, 1])
    inner_left = jnp.logical_and(lane >= 124, has[0, -1])
    inner_lanes = jnp.logical_or(inner_right, inner_left)
    inner_below = jnp.logical_and(low, has[1, 0])
    inner_above = jnp.logical_and(sub >= 4, has[-1, 0])
    inner_subs = jnp.logical_or(inner_below, inner_above)
    inner_both = jnp.logical_and(inner_subs, inner_lanes)
    sub_mask = inner_subs.astype(jnp.float32)
    lane_mask = inner_lanes.astype(jnp.float32)
    beyond_edge = jnp.logical_and(last_lane, jnp.logical_not(has[0, 1]))
    edge_mask = jnp.where(beyond_edge, 0.0, 1.0)
    moved_lanes = jnp.logical_or(
        jnp.logical_or(jnp.logical_and(lane < 3, has[0, 1]), last_lane),
        jnp.logical_and(jnp.logical_and(lane >= 123, lane < 127), has[0, -1]),
    )
    moved_mask = moved_lanes.astype(jnp.float32)
    halo = slice(rows, rows + 8)
    again = slice(rows + 8, rows + 16)
    zero = jnp.zeros((8, 128), jnp.float32)
    everywhere = tuple(range(SIDE))

    def stresses(level, base, where, energy=None):
        r, rr, s = pl.ds(base, 8), pl.ds(base + 1, 8), pl.ds(base + 8, 8)
        for k in where:
            d = []
            for c in range(2):
                u = vl[level, c, k, rr, :] - v[level, c, k, r, :]
                w = v[level, c, k, rr, :] - vl[level, c, k, r, :]
                d.append((u + w, u - w))
            (dx0, dy0), (dx1, dy1) = d
            volume, shear = dx0 + dy1, dy0 + dx1
            common = moduli[0, k, r, :] * volume
            twice = moduli[1, k, r, :]
            xx, xy, yy = common + twice * dx0, moduli[2, k, r, :] * shear, common + twice * dy1
            if energy is not None and k < extra:
                energy = energy + (xx * dx0 + yy * dy1 + xy * shear)
            stress[level, 0, k, s, :] = xx
            stress[level, 1, k, s, :] = xy
            stress[level, 2, k, s, :] = yy
        return energy

    def row_before(level):
        for q in range(3):
            for k in range(SIDE):
                stress[level, q, k, 0:8, :] = stress[level, q, k, rows + 8 : rows + 16, :]

    def forces(level, base, acc, where, border=False, final=False, span=SIDE, counted=range(SIDE - 1)):
        r, s, b = pl.ds(base, 8), pl.ds(base + 8, 8), pl.ds(base + 7, 8)
        before = {(k - 1) % span for k in where}
        behind = set() if final else {(k + 1) % span for k in where}
        plain, moved = ({}, {}), ({}, {})
        for k in sorted(before | behind | set(where)):
            xx, xy, yy = stress[level, 0, k, s, :], stress[level, 1, k, s, :], stress[level, 2, k, s, :]
            xx_b, xy_b, yy_b = stress[level, 0, k, b, :], stress[level, 1, k, b, :], stress[level, 2, k, b, :]
            dxx, sxy, dxy, syy = xx_b - xx, xy_b + xy, xy_b - xy, yy_b + yy
            if k in where or k in behind:
                plain[0][k] = dxx - sxy
                plain[1][k] = dxy - syy
            if k in where or k in before:
                moved[0][k] = dxx + sxy
                moved[1][k] = dxy + syy
        for c in range(2):
            turned = {k: pltpu.roll(x, 1, 1) for k, x in moved[c].items()}
            returned = {} if final else {k: pltpu.roll(x, 127, 1) for k, x in plain[c].items()}
            for k in where:
                old = v[level, c, k, r, :]
                value = plain[c][k] + jnp.where(first_lane, turned[(k - 1) % span], turned[k])
                if level:
                    value = value - old
                if final:
                    v[level + 1, c, k, r, :] = value
                    continue
                after = jnp.where(last_lane, returned[(k + 1) % span], returned[k]) + moved[c][k]
                if level:
                    after = after - vl[level, c, k, r, :]
                if border:
                    value, after = value * sub_mask, after * sub_mask
                if k == extra:
                    value, after = value * lane_mask, after * moved_mask
                elif k == extra - 1:
                    after = after * edge_mask
                if acc is not None and k in counted:
                    acc = (acc[0] + old * value, acc[1] + value * value)
                v[level + 1, c, k, r, :] = value
                vl[level + 1, c, k, r, :] = after
        return acc

    def vector_done(level, acc):
        for c in range(2):
            for k in range(SIDE):
                v[level + 1, c, k, again, :] = v[level + 1, c, k, 0:8, :]
                vl[level + 1, c, k, again, :] = vl[level + 1, c, k, 0:8, :]
        moments[2 * level + 1] = acc[0]
        moments[2 * level + 2] = acc[1]

    def rows_from(t):
        return pl.multiple_of(8 * t, 8)

    inside = tuple(range(1, planes - 1))
    outside = tuple(k for k in everywhere if k not in inside)

    edges = (0, 1, tiles - 2, tiles - 1)

    def inner_stresses(level, first):
        def step(t, carry):
            stresses(level, rows_from(t + first), range(planes))
            return carry

        loop(tiles - 1 - first, step, 0)

    def inner_forces(level):
        forces(level, 8, None, range(planes), span=planes)
        acc = loop(
            tiles - 4,
            lambda t, acc: forces(level, rows_from(t + 2), acc, range(planes), span=planes, counted=inside),
            (zero, zero),
        )
        forces(level, 8 * (tiles - 2), None, range(planes), span=planes)
        moments[2 * level + 1] = acc[0]
        moments[2 * level + 2] = acc[1]

    last = LEVELS - 1
    inner_stresses(0, 0)
    inner_forces(0)
    inner_stresses(1, 1)
    inner_forces(1)
    pl.semaphore_wait(met.at[0], len(WAYS))
    for dx, dy in WAYS:
        pl.semaphore_signal(met.at[1], inc=1, device_id=at(2 * dx, 2 * dy), device_id_type=MESH)

    for level in range(2, last):
        inner_stresses(level, 1)
        inner_forces(level)
    moments[2 * LEVELS - 1] = loop(
        tiles - 4, lambda t, energy: stresses(last, rows_from(t + 2), inside, energy), zero
    )

    def arrived(ways):
        for index in range(len(WAYS)):
            dx, dy = WAYS[index]
            if (dx, dy) in ways:
                @pl.when(has[-dx, -dy])
                def _(index=index):
                    for copy in copies(index):
                        copy.wait_recv()

    def beside_moduli(part):
        left, right = looked_up(mat_halo[0, part, :]), looked_up(mat_halo[2, part, :])
        size = part.stop - part.start
        wide_lane = lax.broadcasted_iota(jnp.int32, (size, 128), 1)
        for q in range(2):
            near = jnp.broadcast_to(right[q][:, 0:1], (size, 128))
            far = jnp.broadcast_to(left[q][:, mat_cols - 1 : mat_cols], (size, 128))
            compact[q, part, :] = jnp.where(wide_lane < 64, near, far)

    arrived([(0, -1), (0, 1)])
    for c in range(2):
        beside = col_halo[c].T
        for t in range(tiles):
            v[0, c, extra, 8 * t : 8 * t + 8, :] = jnp.where(inner_lanes, beside[8 * t : 8 * t + 8], 0.0)
    beside_moduli(slice(0, mat_rows))
    for t in range(tiles):
        lam, mu = (
            jnp.where(inner_lanes, jnp.broadcast_to(compact[q, t : t + 1, :], (8, 128)), 0.0) for q in range(2)
        )
        put_moduli((extra, slice(8 * t, 8 * t + 8)), lam, mu)

    def rest_shift(t, carry):
        r = pl.ds(rows_from(t), 8)
        for c in range(2):
            near, far, start = (v[0, c, k, r, :] for k in (planes - 1, extra, 0))
            for k, value in enumerate(shifted_left([near, far, start])[:-1]):
                vl[0, c, planes - 1 + k, r, :] = value
        return carry

    loop(tiles, rest_shift, 0)

    def stress_outside(t, carry):
        stresses(0, rows_from(t), (planes - 1, extra))
        return carry

    loop(tiles - 1, stress_outside, 0)
    acc = loop(
        tiles - 4, lambda t, acc: forces(0, rows_from(t + 2), acc, outside), (moments[1], moments[2])
    )

    arrived([way for way in WAYS if way[0]])
    for c in range(2):
        for k in range(planes):
            part = slice(128 * k, 128 * (k + 1))
            ring = jnp.where(low, row_halo[0, c, :, part], row_halo[1, c, :, part])
            v[0, c, k, halo, :] = jnp.where(inner_subs, ring, 0.0)
        below = jnp.where(left_lanes, corner[0, 1, c], corner[0, 0, c])
        above = jnp.where(left_lanes, corner[1, 1, c], corner[1, 0, c])
        v[0, c, extra, halo, :] = jnp.where(inner_both, jnp.where(low, below, above), 0.0)
        for k in range(SIDE):
            v[0, c, k, again, :] = v[0, c, k, 0:8, :]
    beyond = widened(mat_halo[1, mat_rows : mat_rows + 16, :])
    for k in range(planes):
        part = slice(128 * k, 128 * (k + 1))
        lam, mu = (
            jnp.where(
                inner_subs,
                jnp.where(low, jnp.broadcast_to(m[0:1, part], (8, 128)), jnp.broadcast_to(m[15:16, part], (8, 128))),
                0.0,
            )
            for m in beyond
        )
        put_moduli((k, halo), lam, mu)
    beside_moduli(slice(mat_rows, mat_rows + 16))
    lam, mu = (
        jnp.where(
            inner_both,
            jnp.where(
                low,
                jnp.broadcast_to(compact[q, mat_rows : mat_rows + 1, :], (8, 128)),
                jnp.broadcast_to(compact[q, mat_rows + 15 : mat_rows + 16, :], (8, 128)),
            ),
            0.0,
        )
        for q in range(2)
    )
    put_moduli((extra, halo), lam, mu)
    for c in range(2):
        for k, value in enumerate(shifted_left([v[0, c, k, halo, :] for k in range(SIDE)])):
            vl[0, c, k, halo, :] = value
        for k in range(SIDE):
            vl[0, c, k, again, :] = vl[0, c, k, 0:8, :]
    stresses(0, rows - 8, everywhere)
    stresses(0, rows, everywhere)
    row_before(0)
    for t in edges:
        acc = forces(0, 8 * t, acc, everywhere)
    forces(0, rows, None, everywhere, border=True)
    vector_done(0, acc)

    def outer_stresses(level, energy):
        energy = loop(
            tiles - 4, lambda t, energy: stresses(level, rows_from(t + 2), outside, energy), energy
        )
        for t in edges:
            energy = stresses(level, 8 * t, everywhere, energy)
        stresses(level, rows, everywhere)
        row_before(level)
        return energy

    for level in range(1, last):
        outer_stresses(level, None)
        acc = loop(
            tiles - 4,
            lambda t, acc, level=level: forces(level, rows_from(t + 2), acc, outside),
            (moments[2 * level + 1], moments[2 * level + 2]),
        )
        for t in edges:
            acc = forces(level, 8 * t, acc, everywhere)
        forces(level, rows, None, everywhere, border=True)
        vector_done(level, acc)
    energy = outer_stresses(last, moments[2 * LEVELS - 1])
    moments[2 * LEVELS - 1] = energy + DIAG * moments[2 * LEVELS - 2]

    partial = jnp.sum(moments[0 : 2 * LEVELS], axis=1)
    partial = jnp.sum(partial, axis=1, keepdims=True)
    mine = jnp.sum(jnp.where(lane == sub, jnp.broadcast_to(partial, (8, 128)), 0.0), axis=0, keepdims=True)
    me = gx * ny + gy
    own_sum[0] = mine
    slots[me] = mine
    pl.semaphore_wait(met.at[1], len(WAYS))
    peers = [(a, b) for a in range(nx) for b in range(ny) if a or b]
    peers.sort(key=lambda w: -2 * min(w[1], ny - w[1]) - min(w[0], nx - w[0]))
    for way in peers:
        pltpu.make_async_remote_copy(
            src_ref=own_sum.at[0], dst_ref=slots.at[me], send_sem=sum_send.at[0], recv_sem=sum_recv.at[0],
            device_id=at(*way), device_id_type=MESH,
        ).start()
    everything = pltpu.make_async_remote_copy(
        src_ref=slots.at[0 : nx * ny - 1], dst_ref=slots.at[0 : nx * ny - 1],
        send_sem=sum_send.at[0], recv_sem=sum_recv.at[0], device_id=at(1, 0), device_id_type=MESH,
    )

    def final_forces(t, carry):
        forces(last, rows_from(t), None, range(planes), final=True)
        return carry

    loop(tiles, final_forces, 0)
    everything.wait_recv()
    mine = jnp.sum(slots[...], axis=0)

    g = [jnp.broadcast_to(mine[:, k : k + 1], (8, 128)) for k in range(2 * LEVELS)]
    m = [g[0], g[1]]
    for k in range(2, 2 * LEVELS):
        m.append(g[k] + DIAG * m[k - 1])
    sigma0 = jnp.full((8, 128), MASS, jnp.float32)
    sigma = sigma0 + (CENTRE / SPREAD) * inv_s
    shift = [sigma0] + [sigma] * (2 * LEVELS - 2)
    rho, phi = dict(enumerate(m)), dict(enumerate(m))
    one, nil = jnp.ones((8, 128), jnp.float32), jnp.zeros((8, 128), jnp.float32)
    r_of, p_of, x_of = [one] + [nil] * LEVELS, [one] + [nil] * LEVELS, [nil] * LEVELS
    for t in range(ITERS):
        psi = {l: phi[l + 1] * inv_s + shift[l] * phi[l] for l in range(t, 2 * LEVELS - 1 - t)}
        alpha = rho[t] / psi[t]
        for k in range(t + 1):
            x_of[k] = x_of[k] + alpha * p_of[k]
        ap = [
            (p_of[k - 1] * inv_s if k else nil) + (shift[k] * p_of[k] if k <= t else nil) for k in range(t + 2)
        ]
        for k in range(t + 2):
            r_of[k] = r_of[k] - alpha * ap[k]
        if t + 1 < ITERS:
            new = {l: rho[l] - alpha * psi[l] for l in range(t + 1, 2 * LEVELS - 1 - t)}
            beta = -(alpha * inv_s) * new[t + 1] / rho[t]
            phi = {l: new[l] + beta * phi[l] for l in new}
            rho = new
            for k in range(t + 2):
                p_of[k] = r_of[k] + beta * p_of[k]

    for k in range(LEVELS):
        factors[k] = x_of[k]
    for k in range(LEVELS + 1):
        factors[LEVELS + k] = r_of[k]

    for index in range(len(WAYS)):
        @pl.when(has[WAYS[index]])
        def _(index=index):
            for copy in copies(index):
                copy.wait_send()
    everything.wait_send()


def combine(v, factors, out_x, out_r, x_part, r_part, sems):
    rows, cols = out_x.shape[2], out_x.shape[3]
    planes = cols // 128
    x_of = [factors[k] for k in range(LEVELS)]
    r_of = [factors[LEVELS + k] for k in range(LEVELS + 1)]
    size = rows // PIECES
    copies = []
    for piece in range(PIECES):
        def body(t, carry):
            r = pl.ds(pl.multiple_of(piece * size + 8 * t, 8), 8)
            for c in range(2):
                for k in range(planes):
                    basis = [v[l, c, k, r, :] for l in range(LEVELS + 1)]
                    part = slice(128 * k, 128 * (k + 1))
                    x = x_of[0] * basis[0]
                    for l in range(1, LEVELS):
                        x = x + x_of[l] * basis[l]
                    res = r_of[0] * basis[0]
                    for l in range(1, LEVELS + 1):
                        res = res + r_of[l] * basis[l]
                    x_part[0, c, r, part] = x
                    r_part[0, c, r, part] = res
            return carry

        loop(size // 8, body, 0)
        here = pl.ds(piece * size, size)
        for i, (source, target) in enumerate(((x_part, out_x), (r_part, out_r))):
            copy = pltpu.make_async_copy(source.at[0, :, here, :], target.at[0, :, here, :], sems.at[i, piece])
            copy.start()
            copies.append(copy)
    for copy in copies:
        copy.wait()


def on_device(nx, ny, load, material, lame_table):
    rows, cols = load.shape[2], load.shape[3]
    mat_rows, mat_cols = material.shape[1], material.shape[2]
    planes = cols // 128
    vmem = pl.BlockSpec(memory_space=pltpu.VMEM)
    f32 = jnp.float32
    v, factors = pl.pallas_call(
        functools.partial(kernel, nx, ny),
        out_shape=[
            jax.ShapeDtypeStruct((LEVELS + 1, 2, planes + 1, rows + 16, 128), f32),
            jax.ShapeDtypeStruct((2 * LEVELS + 1, 8, 128), f32),
        ],
        in_specs=[pl.BlockSpec(memory_space=pltpu.HBM)] * 3,
        out_specs=[vmem, vmem],
        scratch_shapes=[
            pltpu.VMEM(load.shape, f32),
            pltpu.VMEM(material.shape, jnp.int32),
            pltpu.SMEM(lame_table.shape, f32),
            pltpu.VMEM((LEVELS, 2, planes + 1, rows + 16, 128), f32),
            pltpu.VMEM((LEVELS, 3, planes + 1, rows + 16, 128), f32),
            pltpu.VMEM((3, planes + 1, rows + 8, 128), f32),
            pltpu.VMEM((2, mat_rows + 16, 128), f32),
            pltpu.VMEM((2, 2, 8, cols), f32),
            pltpu.VMEM((2, 2, 8, 128), f32),
            pltpu.VMEM((2, 128, rows), f32),
            pltpu.VMEM((2, 2, 2, 8, 128), f32),
            pltpu.VMEM((3, mat_rows + 16, mat_cols), jnp.int32),
            pltpu.VMEM((nx * ny, 1, 128), f32),
            pltpu.VMEM((1, 1, 128), f32),
            pltpu.VMEM((2 * LEVELS, 8, 128), f32),
            pltpu.SemaphoreType.DMA((3,)),
            pltpu.SemaphoreType.DMA((2 * len(WAYS),)),
            pltpu.SemaphoreType.DMA((2 * len(WAYS),)),
            pltpu.SemaphoreType.DMA((1,)),
            pltpu.SemaphoreType.DMA((1,)),
            pltpu.SemaphoreType.REGULAR((2,)),
        ],
        compiler_params=pltpu.CompilerParams(
            collective_id=0, has_side_effects=True, vmem_limit_bytes=24 * 1024 * 1024
        ),
    )(*(pltpu.with_memory_space_constraint(a, pltpu.HBM) for a in (load, material, lame_table)))
    return pl.pallas_call(
        combine,
        out_shape=[jax.ShapeDtypeStruct(load.shape, f32)] * 2,
        in_specs=[vmem, vmem],
        out_specs=[pl.BlockSpec(memory_space=pltpu.HBM)] * 2,
        scratch_shapes=[
            pltpu.VMEM(load.shape, f32), pltpu.VMEM(load.shape, f32), pltpu.SemaphoreType.DMA((2, PIECES)),
        ],
        compiler_params=pltpu.CompilerParams(vmem_limit_bytes=24 * 1024 * 1024),
    )(v, factors)


def solution(mesh):
    return jax.shard_map(
        functools.partial(on_device, mesh.shape["gx"], mesh.shape["gy"]),
        mesh=mesh,
        in_specs=(P("samp", None, "gx", "gy"), P("samp", "gx", "gy"), P()),
        out_specs=(P("samp", None, "gx", "gy"), P("samp", None, "gx", "gy")),
        check_vma=False,
    )
```

```python
import functools

import jax
import jax.numpy as jnp
from jax import lax
from jax.experimental import pallas as pl
from jax.experimental.pallas import tpu as pltpu
from jax.sharding import PartitionSpec as P

TILE = 8
CLASSES = 8
ITERS = 4
LEVELS = ITERS
MASS = 0.05
SPREAD = 1.5
CENTRE = 1.5
DIAG = -CENTRE / SPREAD
MESH = pl.DeviceIdType.MESH
WAYS = [(dx, dy) for dx in (-1, 0, 1) for dy in (-1, 0, 1) if (dx, dy) != (0, 0)]
SIDE = 5
PIECES = 4
DIAGONAL = [w for w in WAYS if w[0] and w[1]]


def loop(count, body, carry, unroll=None):
    return lax.fori_loop(0, count, body, carry, unroll=count if unroll is None else unroll)


def kernel(
    nx, ny, load_in, material_in, table_in, v, factors,
    load, material, table, vl, stress, moduli, compact, row_halo, col_send, col_halo, corner, mat_halo, slots,
    own_sum, moments, load_sem, send_sem, recv_sem, sum_send, sum_recv, met,
):
    rows, cols = load.shape[2], load.shape[3]
    tiles, planes = rows // 8, cols // 128
    mat_rows, mat_cols = material.shape[1], material.shape[2]
    extra = planes
    gx, gy = lax.axis_index("gx"), lax.axis_index("gy")
    has = {
        (-1, 0): gx > 0, (1, 0): gx < nx - 1, (0, -1): gy > 0, (0, 1): gy < ny - 1,
    }
    for dx, dy in DIAGONAL:
        has[dx, dy] = jnp.logical_and(has[dx, 0], has[0, dy])

    def at(dx, dy):
        return {"gx": lax.rem(gx + dx + nx, nx), "gy": lax.rem(gy + dy + ny, ny)}

    fetches = [
        pltpu.make_async_copy(load_in, load, load_sem.at[0]),
        pltpu.make_async_copy(material_in, material, load_sem.at[1]),
        pltpu.make_async_copy(table_in, table, load_sem.at[2]),
    ]
    fetches[0].start()
    barrier = pltpu.get_barrier_semaphore()
    for way in sorted(WAYS, key=lambda w: -abs(w[0]) - 2 * abs(w[1])):
        pl.semaphore_signal(barrier, inc=1, device_id=at(*way), device_id_type=MESH)
    fetches[1].start()
    fetches[2].start()
    fetches[0].wait()

    sub = lax.broadcasted_iota(jnp.int32, (8, 128), 0)
    lane = lax.broadcasted_iota(jnp.int32, (8, 128), 1)

    for c in range(2):
        col_send[0, c] = load[0, c, :, 0:128].T[0:8]
        col_send[1, c] = load[0, c, :, cols - 128 : cols].T[120:128]

    fetches[1].wait()
    pl.semaphore_wait(barrier, len(WAYS))

    def copies(index):
        dx, dy = WAYS[index]
        width = slice(0, cols) if dy == 0 else (slice(0, 128) if dy < 0 else slice(cols - 128, cols))
        strip = slice(0, 8) if dx < 0 else slice(rows - 8, rows)
        third = 1 - dy
        if dx == 0:
            mat_src, mat_rows_at = slice(0, mat_rows), slice(0, mat_rows)
            src = col_send.at[0 if dy < 0 else 1]
            dst = col_halo.at[:, slice(0, 8) if dy < 0 else slice(120, 128), :]
        else:
            mat_src = slice(0, 8) if dx < 0 else slice(mat_rows - 8, mat_rows)
            mat_rows_at = slice(mat_rows, mat_rows + 8) if dx < 0 else slice(mat_rows + 8, mat_rows + 16)
            src = load.at[0, :, strip, width]
            if dy == 0:
                dst = row_halo.at[0 if dx < 0 else 1]
            else:
                dst = corner.at[0 if dx < 0 else 1, 0 if dy > 0 else 1]
        field = pltpu.make_async_remote_copy(
            src_ref=src, dst_ref=dst, send_sem=send_sem.at[2 * index], recv_sem=recv_sem.at[2 * index],
            device_id=at(dx, dy), device_id_type=MESH,
        )
        classes = pltpu.make_async_remote_copy(
            src_ref=material.at[0, mat_src, :], dst_ref=mat_halo.at[third, mat_rows_at, :],
            send_sem=send_sem.at[2 * index + 1], recv_sem=recv_sem.at[2 * index + 1],
            device_id=at(dx, dy), device_id_type=MESH,
        )
        return field, classes

    order = sorted(range(len(WAYS)), key=lambda i: -abs(WAYS[i][0]) - abs(WAYS[i][1]) - abs(WAYS[i][1]))
    for index in order:
        @pl.when(has[WAYS[index]])
        def _(index=index):
            for copy in copies(index):
                copy.start()

    for way in WAYS:
        pl.semaphore_signal(met.at[0], inc=1, device_id=at(*way), device_id_type=MESH)

    fetches[2].wait()
    mean = 0.0
    for k in range(CLASSES):
        mean = mean + (table[0, k] + 3.0 * table[1, k])
    inv_s = jnp.full((8, 128), (SPREAD / CLASSES) * mean, jnp.float32)
    quarter = 0.25 / inv_s

    def looked_up(classes):
        lam = jnp.zeros(classes.shape, jnp.float32)
        mu = jnp.zeros(classes.shape, jnp.float32)
        for k in range(CLASSES):
            hit = classes == k
            lam = jnp.where(hit, table[0, k], lam)
            mu = jnp.where(hit, table[1, k], mu)
        return lam, mu

    spread_row = lax.broadcasted_iota(jnp.int32, (mat_cols, cols), 0)
    spread_col = lax.broadcasted_iota(jnp.int32, (mat_cols, cols), 1)
    spread = (spread_row == spread_col // TILE).astype(jnp.float32)

    def widened(classes):
        lam, mu = looked_up(classes)
        both = jnp.concatenate([lam, mu], axis=0)
        wide = jnp.dot(both, spread, precision=lax.Precision.HIGHEST, preferred_element_type=jnp.float32)
        return wide[: classes.shape[0]], wide[classes.shape[0] :]

    def put_moduli(place, lam, mu):
        k, r = place
        small = quarter * mu
        moduli[0, k, r, :] = quarter * lam
        moduli[1, k, r, :] = small + small
        moduli[2, k, r, :] = small

    lam, mu = widened(material[0])
    for t in range(tiles):
        for k in range(planes):
            part = slice(128 * k, 128 * (k + 1))
            put_moduli(
                (k, slice(8 * t, 8 * t + 8)),
                jnp.broadcast_to(lam[t : t + 1, part], (8, 128)),
                jnp.broadcast_to(mu[t : t + 1, part], (8, 128)),
            )

    def own(t, acc):
        r = pl.ds(pl.multiple_of(8 * t, 8), 8)
        for c in range(2):
            for k in range(planes):
                value = load[0, c, r, 128 * k : 128 * (k + 1)]
                v[0, c, k, r, :] = value
                acc = acc + value * value
        return acc

    moments[0] = loop(tiles, own, jnp.zeros((8, 128), jnp.float32))

    last_lane, first_lane = lane == 127, lane == 0

    def shifted_left(parts):
        turned = [pltpu.roll(x, 127, 1) for x in parts]
        return [jnp.where(last_lane, turned[(k + 1) % len(parts)], turned[k]) for k in range(len(parts))]

    def first_shift(t, carry):
        r = pl.ds(pl.multiple_of(8 * t, 8), 8)
        for c in range(2):
            for k, value in enumerate(shifted_left([v[0, c, k, r, :] for k in range(planes)])):
                vl[0, c, k, r, :] = value
        return carry

    loop(tiles, first_shift, 0)

    low = sub < 4
    left_lanes = lane < 64
    inner_right = jnp.logical_and(lane < 4, has[0, 1])
    inner_left = jnp.logical_and(lane >= 124, has[0, -1])
    inner_lanes = jnp.logical_or(inner_right, inner_left)
    inner_below = jnp.logical_and(low, has[1, 0])
    inner_above = jnp.logical_and(sub >= 4, has[-1, 0])
    inner_subs = jnp.logical_or(inner_below, inner_above)
    inner_both = jnp.logical_and(inner_subs, inner_lanes)
    sub_mask = inner_subs.astype(jnp.float32)
    lane_mask = inner_lanes.astype(jnp.float32)
    beyond_edge = jnp.logical_and(last_lane, jnp.logical_not(has[0, 1]))
    edge_mask = jnp.where(beyond_edge, 0.0, 1.0)
    moved_lanes = jnp.logical_or(
        jnp.logical_or(jnp.logical_and(lane < 3, has[0, 1]), last_lane),
        jnp.logical_and(jnp.logical_and(lane >= 123, lane < 127), has[0, -1]),
    )
    moved_mask = moved_lanes.astype(jnp.float32)
    halo = slice(rows, rows + 8)
    again = slice(rows + 8, rows + 16)
    zero = jnp.zeros((8, 128), jnp.float32)
    everywhere = tuple(range(SIDE))

    def stresses(level, base, where, energy=None):
        r, rr, s = pl.ds(base, 8), pl.ds(base + 1, 8), pl.ds(base + 8, 8)
        for k in where:
            d = []
            for c in range(2):
                u = vl[level, c, k, rr, :] - v[level, c, k, r, :]
                w = v[level, c, k, rr, :] - vl[level, c, k, r, :]
                d.append((u + w, u - w))
            (dx0, dy0), (dx1, dy1) = d
            volume, shear = dx0 + dy1, dy0 + dx1
            common = moduli[0, k, r, :] * volume
            twice = moduli[1, k, r, :]
            xx, xy, yy = common + twice * dx0, moduli[2, k, r, :] * shear, common + twice * dy1
            if energy is not None and k < extra:
                energy = energy + (xx * dx0 + yy * dy1 + xy * shear)
            stress[level, 0, k, s, :] = xx
            stress[level, 1, k, s, :] = xy
            stress[level, 2, k, s, :] = yy
        return energy

    def row_before(level):
        for q in range(3):
            for k in range(SIDE):
                stress[level, q, k, 0:8, :] = stress[level, q, k, rows + 8 : rows + 16, :]

    def forces(level, base, acc, where, border=False, final=False, span=SIDE, counted=range(SIDE - 1)):
        r, s, b = pl.ds(base, 8), pl.ds(base + 8, 8), pl.ds(base + 7, 8)
        before = {(k - 1) % span for k in where}
        behind = set() if final else {(k + 1) % span for k in where}
        plain, moved = ({}, {}), ({}, {})
        for k in sorted(before | behind | set(where)):
            xx, xy, yy = stress[level, 0, k, s, :], stress[level, 1, k, s, :], stress[level, 2, k, s, :]
            xx_b, xy_b, yy_b = stress[level, 0, k, b, :], stress[level, 1, k, b, :], stress[level, 2, k, b, :]
            dxx, sxy, dxy, syy = xx_b - xx, xy_b + xy, xy_b - xy, yy_b + yy
            if k in where or k in behind:
                plain[0][k] = dxx - sxy
                plain[1][k] = dxy - syy
            if k in where or k in before:
                moved[0][k] = dxx + sxy
                moved[1][k] = dxy + syy
        for c in range(2):
            turned = {k: pltpu.roll(x, 1, 1) for k, x in moved[c].items()}
            returned = {} if final else {k: pltpu.roll(x, 127, 1) for k, x in plain[c].items()}
            for k in where:
                old = v[level, c, k, r, :]
                value = plain[c][k] + jnp.where(first_lane, turned[(k - 1) % span], turned[k])
                if level:
                    value = value - old
                if final:
                    v[level + 1, c, k, r, :] = value
                    continue
                after = jnp.where(last_lane, returned[(k + 1) % span], returned[k]) + moved[c][k]
                if level:
                    after = after - vl[level, c, k, r, :]
                if border:
                    value, after = value * sub_mask, after * sub_mask
                if k == extra:
                    value, after = value * lane_mask, after * moved_mask
                elif k == extra - 1:
                    after = after * edge_mask
                if acc is not None and k in counted:
                    acc = (acc[0] + old * value, acc[1] + value * value)
                v[level + 1, c, k, r, :] = value
                vl[level + 1, c, k, r, :] = after
        return acc

    def vector_done(level, acc):
        for c in range(2):
            for k in range(SIDE):
                v[level + 1, c, k, again, :] = v[level + 1, c, k, 0:8, :]
                vl[level + 1, c, k, again, :] = vl[level + 1, c, k, 0:8, :]
        moments[2 * level + 1] = acc[0]
        moments[2 * level + 2] = acc[1]

    def rows_from(t):
        return pl.multiple_of(8 * t, 8)

    inside = tuple(range(1, planes - 1))
    outside = tuple(k for k in everywhere if k not in inside)

    edges = (0, 1, tiles - 2, tiles - 1)

    def inner_stresses(level, first):
        def step(t, carry):
            stresses(level, rows_from(t + first), range(planes))
            return carry

        loop(tiles - 1 - first, step, 0)

    def inner_forces(level):
        forces(level, 8, None, range(planes), span=planes)
        acc = loop(
            tiles - 4,
            lambda t, acc: forces(level, rows_from(t + 2), acc, range(planes), span=planes, counted=inside),
            (zero, zero),
        )
        forces(level, 8 * (tiles - 2), None, range(planes), span=planes)
        moments[2 * level + 1] = acc[0]
        moments[2 * level + 2] = acc[1]

    last = LEVELS - 1
    inner_stresses(0, 0)
    inner_forces(0)
    inner_stresses(1, 1)
    inner_forces(1)
    pl.semaphore_wait(met.at[0], len(WAYS))
    for dx, dy in WAYS:
        pl.semaphore_signal(met.at[1], inc=1, device_id=at(2 * dx, 2 * dy), device_id_type=MESH)

    for level in range(2, last):
        inner_stresses(level, 1)
        inner_forces(level)
    moments[2 * LEVELS - 1] = loop(
        tiles - 4, lambda t, energy: stresses(last, rows_from(t + 2), inside, energy), zero
    )

    def arrived(ways):
        for index in range(len(WAYS)):
            dx, dy = WAYS[index]
            if (dx, dy) in ways:
                @pl.when(has[-dx, -dy])
                def _(index=index):
                    for copy in copies(index):
                        copy.wait_recv()

    def beside_moduli(part):
        left, right = looked_up(mat_halo[0, part, :]), looked_up(mat_halo[2, part, :])
        size = part.stop - part.start
        wide_lane = lax.broadcasted_iota(jnp.int32, (size, 128), 1)
        for q in range(2):
            near = jnp.broadcast_to(right[q][:, 0:1], (size, 128))
            far = jnp.broadcast_to(left[q][:, mat_cols - 1 : mat_cols], (size, 128))
            compact[q, part, :] = jnp.where(wide_lane < 64, near, far)

    arrived([(0, -1), (0, 1)])
    for c in range(2):
        beside = col_halo[c].T
        for t in range(tiles):
            v[0, c, extra, 8 * t : 8 * t + 8, :] = jnp.where(inner_lanes, beside[8 * t : 8 * t + 8], 0.0)
    beside_moduli(slice(0, mat_rows))
    for t in range(tiles):
        lam, mu = (
            jnp.where(inner_lanes, jnp.broadcast_to(compact[q, t : t + 1, :], (8, 128)), 0.0) for q in range(2)
        )
        put_moduli((extra, slice(8 * t, 8 * t + 8)), lam, mu)

    def rest_shift(t, carry):
        r = pl.ds(rows_from(t), 8)
        for c in range(2):
            near, far, start = (v[0, c, k, r, :] for k in (planes - 1, extra, 0))
            for k, value in enumerate(shifted_left([near, far, start])[:-1]):
                vl[0, c, planes - 1 + k, r, :] = value
        return carry

    loop(tiles, rest_shift, 0)

    def stress_outside(t, carry):
        stresses(0, rows_from(t), (planes - 1, extra))
        return carry

    loop(tiles - 1, stress_outside, 0)
    acc = loop(
        tiles - 4, lambda t, acc: forces(0, rows_from(t + 2), acc, outside), (moments[1], moments[2])
    )

    arrived([way for way in WAYS if way[0]])
    for c in range(2):
        for k in range(planes):
            part = slice(128 * k, 128 * (k + 1))
            ring = jnp.where(low, row_halo[0, c, :, part], row_halo[1, c, :, part])
            v[0, c, k, halo, :] = jnp.where(inner_subs, ring, 0.0)
        below = jnp.where(left_lanes, corner[0, 1, c], corner[0, 0, c])
        above = jnp.where(left_lanes, corner[1, 1, c], corner[1, 0, c])
        v[0, c, extra, halo, :] = jnp.where(inner_both, jnp.where(low, below, above), 0.0)
        for k in range(SIDE):
            v[0, c, k, again, :] = v[0, c, k, 0:8, :]
    beyond = widened(mat_halo[1, mat_rows : mat_rows + 16, :])
    for k in range(planes):
        part = slice(128 * k, 128 * (k + 1))
        lam, mu = (
            jnp.where(
                inner_subs,
                jnp.where(low, jnp.broadcast_to(m[0:1, part], (8, 128)), jnp.broadcast_to(m[15:16, part], (8, 128))),
                0.0,
            )
            for m in beyond
        )
        put_moduli((k, halo), lam, mu)
    beside_moduli(slice(mat_rows, mat_rows + 16))
    lam, mu = (
        jnp.where(
            inner_both,
            jnp.where(
                low,
                jnp.broadcast_to(compact[q, mat_rows : mat_rows + 1, :], (8, 128)),
                jnp.broadcast_to(compact[q, mat_rows + 15 : mat_rows + 16, :], (8, 128)),
            ),
            0.0,
        )
        for q in range(2)
    )
    put_moduli((extra, halo), lam, mu)
    for c in range(2):
        for k, value in enumerate(shifted_left([v[0, c, k, halo, :] for k in range(SIDE)])):
            vl[0, c, k, halo, :] = value
        for k in range(SIDE):
            vl[0, c, k, again, :] = vl[0, c, k, 0:8, :]
    stresses(0, rows - 8, everywhere)
    stresses(0, rows, everywhere)
    row_before(0)
    for t in edges:
        acc = forces(0, 8 * t, acc, everywhere)
    forces(0, rows, None, everywhere, border=True)
    vector_done(0, acc)

    def outer_stresses(level, energy):
        energy = loop(
            tiles - 4, lambda t, energy: stresses(level, rows_from(t + 2), outside, energy), energy
        )
        for t in edges:
            energy = stresses(level, 8 * t, everywhere, energy)
        stresses(level, rows, everywhere)
        row_before(level)
        return energy

    for level in range(1, last):
        outer_stresses(level, None)
        acc = loop(
            tiles - 4,
            lambda t, acc, level=level: forces(level, rows_from(t + 2), acc, outside),
            (moments[2 * level + 1], moments[2 * level + 2]),
        )
        for t in edges:
            acc = forces(level, 8 * t, acc, everywhere)
        forces(level, rows, None, everywhere, border=True)
        vector_done(level, acc)
    energy = outer_stresses(last, moments[2 * LEVELS - 1])
    moments[2 * LEVELS - 1] = energy + DIAG * moments[2 * LEVELS - 2]

    partial = jnp.sum(moments[0 : 2 * LEVELS], axis=1)
    partial = jnp.sum(partial, axis=1, keepdims=True)
    mine = jnp.sum(jnp.where(lane == sub, jnp.broadcast_to(partial, (8, 128)), 0.0), axis=0, keepdims=True)
    me = gx * ny + gy
    own_sum[0] = mine
    slots[me] = mine
    pl.semaphore_wait(met.at[1], len(WAYS))
    peers = [(a, b) for a in range(nx) for b in range(ny) if a or b]
    peers.sort(key=lambda w: -2 * min(w[1], ny - w[1]) - min(w[0], nx - w[0]))
    for way in peers:
        pltpu.make_async_remote_copy(
            src_ref=own_sum.at[0], dst_ref=slots.at[me], send_sem=sum_send.at[0], recv_sem=sum_recv.at[0],
            device_id=at(*way), device_id_type=MESH,
        ).start()
    everything = pltpu.make_async_remote_copy(
        src_ref=slots.at[0 : nx * ny - 1], dst_ref=slots.at[0 : nx * ny - 1],
        send_sem=sum_send.at[0], recv_sem=sum_recv.at[0], device_id=at(1, 0), device_id_type=MESH,
    )

    def final_forces(t, carry):
        forces(last, rows_from(t), None, range(planes), final=True)
        return carry

    loop(tiles, final_forces, 0)
    everything.wait_recv()
    lines = [slots[i] for i in range(nx * ny)]
    while len(lines) > 1:
        lines = [lines[i] + lines[i + 1] for i in range(0, len(lines), 2)]
    mine = lines[0]

    g = [jnp.broadcast_to(mine[:, k : k + 1], (8, 128)) for k in range(2 * LEVELS)]
    m = [g[0], g[1]]
    for k in range(2, 2 * LEVELS):
        m.append(g[k] + DIAG * m[k - 1])
    sigma0 = jnp.full((8, 128), MASS, jnp.float32)
    sigma = sigma0 + (CENTRE / SPREAD) * inv_s
    shift = [sigma0] + [sigma] * (2 * LEVELS - 2)
    rho, phi = dict(enumerate(m)), dict(enumerate(m))
    one, nil = jnp.ones((8, 128), jnp.float32), jnp.zeros((8, 128), jnp.float32)
    r_of, p_of, x_of = [one] + [nil] * LEVELS, [one] + [nil] * LEVELS, [nil] * LEVELS
    for t in range(ITERS):
        psi = {l: phi[l + 1] * inv_s + shift[l] * phi[l] for l in range(t, 2 * LEVELS - 1 - t)}
        alpha = rho[t] / psi[t]
        for k in range(t + 1):
            x_of[k] = x_of[k] + alpha * p_of[k]
        ap = [
            (p_of[k - 1] * inv_s if k else nil) + (shift[k] * p_of[k] if k <= t else nil) for k in range(t + 2)
        ]
        for k in range(t + 2):
            r_of[k] = r_of[k] - alpha * ap[k]
        if t + 1 < ITERS:
            new = {l: rho[l] - alpha * psi[l] for l in range(t + 1, 2 * LEVELS - 1 - t)}
            beta = -(alpha * inv_s) * new[t + 1] / rho[t]
            phi = {l: new[l] + beta * phi[l] for l in new}
            rho = new
            for k in range(t + 2):
                p_of[k] = r_of[k] + beta * p_of[k]

    for k in range(LEVELS):
        factors[k] = x_of[k]
    for k in range(LEVELS + 1):
        factors[LEVELS + k] = r_of[k]

    for index in range(len(WAYS)):
        @pl.when(has[WAYS[index]])
        def _(index=index):
            for copy in copies(index):
                copy.wait_send()
    everything.wait_send()


def combine(v, factors, out_x, out_r, x_part, r_part, sems):
    rows, cols = out_x.shape[2], out_x.shape[3]
    planes = cols // 128
    x_of = [factors[k] for k in range(LEVELS)]
    r_of = [factors[LEVELS + k] for k in range(LEVELS + 1)]
    size = rows // PIECES
    copies = []
    for piece in range(PIECES):
        def body(t, carry):
            r = pl.ds(pl.multiple_of(piece * size + 8 * t, 8), 8)
            for c in range(2):
                for k in range(planes):
                    basis = [v[l, c, k, r, :] for l in range(LEVELS + 1)]
                    part = slice(128 * k, 128 * (k + 1))
                    x = x_of[0] * basis[0]
                    for l in range(1, LEVELS):
                        x = x + x_of[l] * basis[l]
                    res = r_of[0] * basis[0]
                    for l in range(1, LEVELS + 1):
                        res = res + r_of[l] * basis[l]
                    x_part[0, c, r, part] = x
                    r_part[0, c, r, part] = res
            return carry

        loop(size // 8, body, 0)
        here = pl.ds(piece * size, size)
        for i, (source, target) in enumerate(((x_part, out_x), (r_part, out_r))):
            copy = pltpu.make_async_copy(source.at[0, :, here, :], target.at[0, :, here, :], sems.at[i, piece])
            copy.start()
            copies.append(copy)
    for copy in copies:
        copy.wait()


def on_device(nx, ny, load, material, lame_table):
    rows, cols = load.shape[2], load.shape[3]
    mat_rows, mat_cols = material.shape[1], material.shape[2]
    planes = cols // 128
    vmem = pl.BlockSpec(memory_space=pltpu.VMEM)
    f32 = jnp.float32
    v, factors = pl.pallas_call(
        functools.partial(kernel, nx, ny),
        out_shape=[
            jax.ShapeDtypeStruct((LEVELS + 1, 2, planes + 1, rows + 16, 128), f32),
            jax.ShapeDtypeStruct((2 * LEVELS + 1, 8, 128), f32),
        ],
        in_specs=[pl.BlockSpec(memory_space=pltpu.HBM)] * 3,
        out_specs=[vmem, vmem],
        scratch_shapes=[
            pltpu.VMEM(load.shape, f32),
            pltpu.VMEM(material.shape, jnp.int32),
            pltpu.SMEM(lame_table.shape, f32),
            pltpu.VMEM((LEVELS, 2, planes + 1, rows + 16, 128), f32),
            pltpu.VMEM((LEVELS, 3, planes + 1, rows + 16, 128), f32),
            pltpu.VMEM((3, planes + 1, rows + 8, 128), f32),
            pltpu.VMEM((2, mat_rows + 16, 128), f32),
            pltpu.VMEM((2, 2, 8, cols), f32),
            pltpu.VMEM((2, 2, 8, 128), f32),
            pltpu.VMEM((2, 128, rows), f32),
            pltpu.VMEM((2, 2, 2, 8, 128), f32),
            pltpu.VMEM((3, mat_rows + 16, mat_cols), jnp.int32),
            pltpu.VMEM((nx * ny, 1, 128), f32),
            pltpu.VMEM((1, 1, 128), f32),
            pltpu.VMEM((2 * LEVELS, 8, 128), f32),
            pltpu.SemaphoreType.DMA((3,)),
            pltpu.SemaphoreType.DMA((2 * len(WAYS),)),
            pltpu.SemaphoreType.DMA((2 * len(WAYS),)),
            pltpu.SemaphoreType.DMA((1,)),
            pltpu.SemaphoreType.DMA((1,)),
            pltpu.SemaphoreType.REGULAR((2,)),
        ],
        compiler_params=pltpu.CompilerParams(
            collective_id=0, has_side_effects=True, vmem_limit_bytes=24 * 1024 * 1024
        ),
    )(*(pltpu.with_memory_space_constraint(a, pltpu.HBM) for a in (load, material, lame_table)))
    return pl.pallas_call(
        combine,
        out_shape=[jax.ShapeDtypeStruct(load.shape, f32)] * 2,
        in_specs=[vmem, vmem],
        out_specs=[pl.BlockSpec(memory_space=pltpu.HBM)] * 2,
        scratch_shapes=[
            pltpu.VMEM(load.shape, f32), pltpu.VMEM(load.shape, f32), pltpu.SemaphoreType.DMA((2, PIECES)),
        ],
        compiler_params=pltpu.CompilerParams(vmem_limit_bytes=24 * 1024 * 1024),
    )(v, factors)


def solution(mesh):
    return jax.shard_map(
        functools.partial(on_device, mesh.shape["gx"], mesh.shape["gy"]),
        mesh=mesh,
        in_specs=(P("samp", None, "gx", "gy"), P("samp", "gx", "gy"), P()),
        out_specs=(P("samp", None, "gx", "gy"), P("samp", None, "gx", "gy")),
        check_vma=False,
    )
```
